8 devices in a mesh: dp: 2 (over z, y), tp: 4 (over x, core).
Axes of the slice: x: 2, y: 2, z: 1, core: 2. Of those that a mesh axis runs over, the one named last changes fastest.
Arguments:
- hidden: bfloat16 [8, 4096, 2048], P('dp', 'tp'), parts along dimension 0
- attn_gain: float32 [2048], replicated
- w_q: bfloat16 [2048, 2048], P(None, 'tp')
- w_k: bfloat16 [2048, 2048], P(None, 'tp')
- w_v: bfloat16 [2048, 2048], P(None, 'tp')
- q_gain: float32 [2048], P('tp')
- k_gain: float32 [2048], P('tp')
- w_o: bfloat16 [2048, 2048], P('tp')
Outputs:
- output 1: bfloat16 [8, 4096, 2048], P('dp', 'tp'), parts along dimension 0
- output 2: bfloat16 [8, 4096, 16, 128], P('dp', None, 'tp'), parts along dimension 0
- output 3: bfloat16 [8, 4096, 16, 128], P('dp', None, 'tp'), parts along dimension 0
There are 2 independent parts. The reference program is written for one: setup_inputs(seed, part) draws one part's arguments, and reference() takes and returns one part's arrays. A program takes and returns all parts, laid end to end along the dimension named above; an argument that names none is the same for every part.
All inputs are finite; a program needn't handle non-finite values.
Results may differ from the reference program's by a relative error of at most 0.00850629.
Values are sent between devices in bfloat16 or wider.
A program may use at most 1 GiB of HBM per device.

```python
import jax
import jax.numpy as jnp
from jax import lax

BATCH_SIZE = 4
SEQ_LEN = 4096
D_MODEL = 2048
N_HEADS = 16
HEAD_DIM = 128


def setup_inputs(seed: int = 0, part: int = 0) -> dict:
    base_key = jax.random.key(seed)
    part_keys = jax.random.split(jax.random.fold_in(base_key, part), 2)
    key_list = jax.random.split(base_key, 9)
    x_noise = jax.random.normal(part_keys[0], (BATCH_SIZE, SEQ_LEN, D_MODEL), jnp.float32)
    x_mean = jax.random.normal(part_keys[1], (BATCH_SIZE, 1, D_MODEL), jnp.float32)
    head_pos = jnp.arange(N_HEADS, dtype=jnp.float32) / max(N_HEADS - 1, 1)
    q_heads = 10.0 ** (head_pos - 0.5) * jax.random.uniform(key_list[0], (N_HEADS,), jnp.float32, 0.8, 1.2)
    k_heads = 10.0 ** (0.5 - head_pos) * jax.random.uniform(key_list[1], (N_HEADS,), jnp.float32, 0.8, 1.2)
    fan_scale = D_MODEL ** -0.5
    w_shape = (D_MODEL, D_MODEL)
    w_q = jax.random.normal(key_list[2], w_shape, jnp.float32) * (fan_scale * jnp.repeat(q_heads, HEAD_DIM))[None, :]
    w_k = jax.random.normal(key_list[3], w_shape, jnp.float32) * (fan_scale * jnp.repeat(k_heads, HEAD_DIM))[None, :]
    w_v = jax.random.normal(key_list[4], w_shape, jnp.float32) * fan_scale
    w_o = jax.random.normal(key_list[5], w_shape, jnp.float32) * fan_scale
    return {
        'hidden': (x_noise + x_mean).astype(jnp.bfloat16),
        'attn_gain': jax.random.uniform(key_list[6], (D_MODEL,), jnp.float32, 0.5, 1.5),
        'w_q': w_q.astype(jnp.bfloat16),
        'w_k': w_k.astype(jnp.bfloat16),
        'w_v': w_v.astype(jnp.bfloat16),
        'q_gain': jax.random.uniform(key_list[7], (D_MODEL,), jnp.float32, 1.5, 3.5),
        'k_gain': jax.random.uniform(key_list[8], (D_MODEL,), jnp.float32, 1.5, 3.5),
        'w_o': w_o.astype(jnp.bfloat16),
    }


def rope_tables(seq_len, head_dim):
    half_dim = head_dim // 2
    inv_freq = 10000.0 ** (-jnp.arange(half_dim, dtype=jnp.float32) * (2.0 / head_dim))
    angles = jnp.arange(seq_len, dtype=jnp.float32)[:, None] * inv_freq[None, :]
    return jnp.cos(angles), jnp.sin(angles)


def apply_rope(heads_in, cos_tab, sin_tab):
    half_dim = heads_in.shape[-1] // 2
    lower_half = heads_in[..., :half_dim]
    upper_half = heads_in[..., half_dim:]
    cos_bcast = cos_tab[None, :, None, :]
    sin_bcast = sin_tab[None, :, None, :]
    return jnp.concatenate([lower_half * cos_bcast - upper_half * sin_bcast, upper_half * cos_bcast + lower_half * sin_bcast], axis=-1)


def reference(hidden, attn_gain, w_q, w_k, w_v, q_gain, k_gain, w_o):
    x_f32 = hidden.astype(jnp.float32)
    inv_rms = lax.rsqrt(jnp.mean(x_f32 * x_f32, axis=-1, keepdims=True) + 1e-5)
    h_rows = (x_f32 * inv_rms * attn_gain).astype(jnp.bfloat16).reshape(BATCH_SIZE * SEQ_LEN, D_MODEL)
    q_raw = jnp.dot(h_rows, w_q, preferred_element_type=jnp.float32).astype(jnp.bfloat16).astype(jnp.float32)
    k_raw = jnp.dot(h_rows, w_k, preferred_element_type=jnp.float32).astype(jnp.bfloat16).astype(jnp.float32)
    v_rows = jnp.dot(h_rows, w_v, preferred_element_type=jnp.float32).astype(jnp.bfloat16)
    q_normed = q_raw * lax.rsqrt(jnp.mean(q_raw * q_raw, axis=-1, keepdims=True) + 1e-5) * q_gain
    k_normed = k_raw * lax.rsqrt(jnp.mean(k_raw * k_raw, axis=-1, keepdims=True) + 1e-5) * k_gain
    cos_tab, sin_tab = rope_tables(SEQ_LEN, HEAD_DIM)
    head_shape = (BATCH_SIZE, SEQ_LEN, N_HEADS, HEAD_DIM)
    q_rot = apply_rope(q_normed.reshape(head_shape), cos_tab, sin_tab).astype(jnp.bfloat16)
    k_rot = apply_rope(k_normed.reshape(head_shape), cos_tab, sin_tab).astype(jnp.bfloat16)
    v_heads = v_rows.reshape(head_shape)
    positions = jnp.arange(SEQ_LEN)
    causal = positions[:, None] >= positions[None, :]
    score_scale = HEAD_DIM ** -0.5

    def one_head(head_args):
        q_head, k_head, v_head = head_args
        scores = jnp.einsum('bqd,bkd->bqk', q_head.astype(jnp.float32), k_head.astype(jnp.float32)) * score_scale
        scores = jnp.where(causal[None], scores, -1e30)
        prob_bf = jax.nn.softmax(scores, axis=-1).astype(jnp.bfloat16)
        head_out = jnp.einsum('bqk,bkd->bqd', prob_bf.astype(jnp.float32), v_head.astype(jnp.float32))
        return head_out.astype(jnp.bfloat16)

    per_head = lax.map(one_head, (jnp.moveaxis(q_rot, 2, 0), jnp.moveaxis(k_rot, 2, 0), jnp.moveaxis(v_heads, 2, 0)))
    attn_rows = jnp.moveaxis(per_head, 0, 2).reshape(BATCH_SIZE * SEQ_LEN, D_MODEL)
    y_rows = jnp.dot(attn_rows, w_o, preferred_element_type=jnp.float32).astype(jnp.bfloat16)
    hidden_out = (x_f32 + y_rows.reshape(hidden.shape).astype(jnp.float32)).astype(jnp.bfloat16)
    return (hidden_out, k_rot, v_heads)
```

```python
import functools
import math

import jax
import jax.numpy as jnp
from jax import lax
from jax.experimental import pallas as pl
from jax.experimental.pallas import tpu as pltpu
from jax.sharding import PartitionSpec as P

HD = 128
LOG2E = math.log2(math.e)
F32 = jnp.float32
BF16 = jnp.bfloat16
VMEM_LIMIT = 60 * 1024 * 1024


def params(*sem):
    return pltpu.CompilerParams(dimension_semantics=sem, vmem_limit_bytes=VMEM_LIMIT)


def cost(flops, nbytes, trans=0):
    return pl.CostEstimate(flops=int(flops), bytes_accessed=int(nbytes), transcendentals=int(trans))


def rope_tables(seq_len):
    half_dim = HD // 2
    inv_freq = 10000.0 ** (-jnp.arange(half_dim, dtype=F32) * (2.0 / HD))
    angles = jnp.arange(seq_len, dtype=F32)[:, None] * inv_freq[None, :]
    c, s = jnp.cos(angles), jnp.sin(angles)
    return jnp.concatenate([c, c], axis=1), jnp.concatenate([-s, s], axis=1)


def sq_sum(a):
    part = None
    for g in range(a.shape[1] // HD):
        t = a[:, g * HD:(g + 1) * HD]
        part = t * t if part is None else part + t * t
    return jnp.sum(part.T, axis=0, keepdims=True)


def spread_heads(scr, blocks):
    n = len(blocks)
    rows = blocks[0].shape[0]
    for g, t in enumerate(blocks):
        scr[pl.ds(g, rows, stride=n), :] = t
    return scr[...].astype(BF16)


def qkv_kernel(h_ref, wq_ref, wk_ref, wv_ref, *refs):
    q_ref, k_ref, v_ref, vc_ref, ss_ref, scr = refs[-6:]
    h = h_ref[...]
    cols = wq_ref.shape[1]
    q = jnp.dot(h, wq_ref[...], preferred_element_type=F32).astype(BF16)
    q_ref[...] = q
    k = jnp.dot(h, wk_ref[...], preferred_element_type=F32).astype(BF16)
    k_ref[...] = k
    ss_ref[0:1, :] = sq_sum(q.astype(F32))
    v = jnp.dot(h, wv_ref[...], preferred_element_type=F32)
    v_ref[...] = v.astype(BF16)
    ss_ref[1:2, :] = sq_sum(k.astype(F32))
    vc_ref[...] = spread_heads(scr, [v[:, g * HD:(g + 1) * HD] for g in range(cols // HD)])


def qkv_call(h, wq, wk, wv, vc_prev, b, n_batch):
    seq, width = h.shape
    cols = wq.shape[1]
    heads = cols // HD
    bq = 512
    nq = seq // bq
    wspec = pl.BlockSpec((width, cols), lambda i: (0, 0))
    rspec = pl.BlockSpec((bq, cols), lambda i: (i, 0))
    in_specs = [pl.BlockSpec((bq, width), lambda i: (i, 0)), wspec, wspec, wspec]
    args = [h, wq, wk, wv]
    aliases = {}
    if vc_prev is not None:
        in_specs.append(pl.BlockSpec(memory_space=pl.ANY))
        args.append(vc_prev)
        aliases = {4: 3}
    base = b * nq
    return pl.pallas_call(
        qkv_kernel,
        grid=(nq,),
        in_specs=in_specs,
        out_specs=[rspec, rspec, rspec, pl.BlockSpec((bq * heads, HD), lambda i: (base + i, 0)), pl.BlockSpec((2, bq), lambda i: (0, i))],
        out_shape=[jax.ShapeDtypeStruct((seq, cols), BF16)] * 3 + [jax.ShapeDtypeStruct((n_batch * seq * heads, HD), BF16), jax.ShapeDtypeStruct((2, seq), F32)],
        scratch_shapes=[pltpu.VMEM((bq * heads, HD), F32)],
        input_output_aliases=aliases,
        compiler_params=params("arbitrary"),
        cost_estimate=cost(6 * seq * width * cols, 2 * (seq * width + 3 * width * cols + 4 * seq * cols)),
        name="qkv",
    )(*args)


def rope_kernel(width, q_ref, k_ref, ss_ref, qg_ref, kg_ref, c_ref, s_ref, *refs):
    qr_ref, kr_ref, kc_ref, scr = refs[-4:]
    ct, st = c_ref[...], s_ref[...]
    rows = q_ref.shape[0]
    inv = lax.rsqrt(ss_ref[...] * (1.0 / width) + 1e-5)
    inv_t = jnp.concatenate([inv, jnp.zeros((6, rows), F32)], axis=0).T

    def turn(x_ref, col, g_ref):
        scale = inv_t[:, col:col + 1]
        outs = []
        for g in range(x_ref.shape[1] // HD):
            sl = slice(g * HD, (g + 1) * HD)
            n = x_ref[:, sl].astype(F32) * scale * g_ref[:, sl]
            outs.append(n * ct + pltpu.roll(n, HD // 2, 1) * st)
        return outs

    for g, t in enumerate(turn(q_ref, 0, qg_ref)):
        qr_ref[:, g * HD:(g + 1) * HD] = t.astype(BF16)
    ks = turn(k_ref, 1, kg_ref)
    for g, t in enumerate(ks):
        kr_ref[:, g * HD:(g + 1) * HD] = t.astype(BF16)
    kc_ref[...] = spread_heads(scr, ks)


def rope_call(q, k, ss, qg, kg, ct, st, kc_prev, b, n_batch, width):
    seq, cols = q.shape
    heads = cols // HD
    bq = 512
    nq = seq // bq
    rspec = pl.BlockSpec((bq, cols), lambda i: (i, 0))
    tspec = pl.BlockSpec((bq, HD), lambda i: (i, 0))
    gspec = pl.BlockSpec((1, cols), lambda i: (0, 0))
    in_specs = [rspec, rspec, pl.BlockSpec((2, bq), lambda i: (0, i)), gspec, gspec, tspec, tspec]
    args = [q, k, ss, qg, kg, ct, st]
    aliases = {}
    if kc_prev is not None:
        in_specs.append(pl.BlockSpec(memory_space=pl.ANY))
        args.append(kc_prev)
        aliases = {7: 2}
    base = b * nq
    return pl.pallas_call(
        functools.partial(rope_kernel, width),
        grid=(nq,),
        in_specs=in_specs,
        out_specs=[rspec, rspec, pl.BlockSpec((bq * heads, HD), lambda i: (base + i, 0))],
        out_shape=[jax.ShapeDtypeStruct((seq, cols), BF16)] * 2 + [jax.ShapeDtypeStruct((n_batch * seq * heads, HD), BF16)],
        scratch_shapes=[pltpu.VMEM((bq * heads, HD), F32)],
        input_output_aliases=aliases,
        compiler_params=params("arbitrary"),
        cost_estimate=cost(7e9, 10 * seq * cols),
        name="rope",
    )(*args)


def attn_kernel(n_h, bq, q_ref, k_ref, v_ref, o_ref, m_s, l_s, acc_s):
    i = pl.program_id(1)
    c = HD ** -0.5 * LOG2E
    nl = bq // HD

    def step(j, first):
        rows = pl.ds(pl.multiple_of(j * bq, bq), bq)
        scores = []
        for g in range(n_h):
            sl = slice(g * HD, (g + 1) * HD)
            s = lax.dot_general(q_ref[:, sl], k_ref[rows, sl], (((1,), (1,)), ((), ())), preferred_element_type=F32)
            if first:
                keep = lax.broadcasted_iota(jnp.int32, (bq, bq), 0) >= lax.broadcasted_iota(jnp.int32, (bq, bq), 1)
                s = jnp.where(keep, s, -1e30)
            scores.append(s)
        for g in range(n_h):
            sl = slice(g * HD, (g + 1) * HD)
            s = scores[g]
            top = jnp.max(s, axis=1, keepdims=True) * c
            if first:
                m_new = jnp.broadcast_to(top, (bq, HD))
            else:
                m_old = m_s[g]
                m_new = jnp.maximum(m_old, top)
            parts = [jnp.exp2(s[:, t * HD:(t + 1) * HD] * c - m_new) for t in range(nl)]
            l_new = functools.reduce(lambda a, b2: a + b2, parts)
            p = jnp.concatenate([t.astype(BF16) for t in parts], axis=1)
            pv = jnp.dot(p, v_ref[rows, sl], preferred_element_type=F32)
            m_s[g] = m_new
            if first:
                l_s[g] = l_new
                acc_s[g] = pv
            else:
                alpha = jnp.exp2(m_old - m_new)
                l_s[g] = l_s[g] * alpha + l_new
                acc_s[g] = acc_s[g] * alpha + pv

    step(i, True)

    def body(j, carry):
        step(j, False)
        return carry

    lax.fori_loop(0, i, body, 0)
    for g in range(n_h):
        l = jnp.sum(l_s[g], axis=1, keepdims=True)
        o_ref[:, g * HD:(g + 1) * HD] = (acc_s[g] / l).astype(BF16)


def attn_call(q, k, v):
    seq, cols = q.shape
    bq = 512
    n_h = 2
    qspec = pl.BlockSpec((bq, n_h * HD), lambda h, i: (i, h))
    kspec = pl.BlockSpec((seq, n_h * HD), lambda h, i: (0, h))
    return pl.pallas_call(
        functools.partial(attn_kernel, n_h, bq),
        grid=(cols // (n_h * HD), seq // bq),
        in_specs=[qspec, kspec, kspec],
        out_specs=qspec,
        out_shape=jax.ShapeDtypeStruct((seq, cols), BF16),
        scratch_shapes=[pltpu.VMEM((n_h, bq, HD), F32)] * 3,
        compiler_params=params("arbitrary", "arbitrary"),
        cost_estimate=cost(4 * seq * seq * cols, 8 * seq * cols, seq * seq * cols // HD // 2),
        name="attn",
    )(q, k, v)


def out_kernel(o0, o1, o2, o3, w0, w1, w2, w3, x_ref, *refs):
    out_ref = refs[-1]
    acc = jnp.dot(o0[...], w0[...], preferred_element_type=F32)
    for o, w in ((o1, w1), (o2, w2), (o3, w3)):
        acc += jnp.dot(o[...], w[...], preferred_element_type=F32)
    y = acc.astype(BF16).astype(F32)
    out_ref[0] = (x_ref[0].astype(F32) + y).astype(BF16)


def out_call(os, ws, x, prev, b):
    n_batch, rows, width = x.shape
    cols = os[0].shape[1]
    bn = 512
    ospec = pl.BlockSpec((rows, cols), lambda n: (0, 0))
    wspec = pl.BlockSpec((cols, bn), lambda n: (0, n))
    xspec = pl.BlockSpec((1, rows, bn), lambda n: (b, 0, n))
    in_specs = [ospec] * 4 + [wspec] * 4 + [xspec]
    args = [*os, *ws, x]
    aliases = {}
    if prev is not None:
        in_specs.append(pl.BlockSpec(memory_space=pl.ANY))
        args.append(prev)
        aliases = {9: 0}
    return pl.pallas_call(
        out_kernel,
        grid=(width // bn,),
        in_specs=in_specs,
        out_specs=xspec,
        out_shape=jax.ShapeDtypeStruct(x.shape, BF16),
        input_output_aliases=aliases,
        compiler_params=params("arbitrary"),
        cost_estimate=cost(2 * rows * width * width, 2 * (width * width + 3 * rows * width)),
        name="outproj",
    )(*args)


def solution(mesh):
    n_tp = mesh.shape['tp']
    pairs = {r: [(d, d ^ r) for d in range(n_tp)] for r in range(1, n_tp)}

    def local_block(x_local, attn_gain, wq, wk, wv, qg, kg, wo_rows):
        n_batch, rows, width = x_local.shape
        seq = rows * n_tp
        cols = wq.shape[1]
        me = lax.axis_index('tp')
        ct, st = rope_tables(seq)

        def exchange(o):
            res = []
            for r in range(n_tp):
                piece = lax.dynamic_slice_in_dim(o, (me ^ r) * rows, rows, axis=0)
                res.append(piece if r == 0 else lax.ppermute(piece, 'tp', pairs[r]))
            return res

        qg, kg = qg.reshape(1, cols), kg.reshape(1, cols)
        hs = []
        for b in range(n_batch):
            xf = x_local[b].astype(F32)
            inv_rms = lax.rsqrt(jnp.mean(xf * xf, axis=-1, keepdims=True) + 1e-5)
            normed = (xf * inv_rms * attn_gain).astype(BF16)
            hs.append(lax.all_gather(normed, 'tp', axis=0, tiled=True))
        vc = kc = out = o_prev = ws = None
        pend = []
        for b in range(n_batch):
            if o_prev is not None:
                hs[b], o_prev = lax.optimization_barrier((hs[b], o_prev))
                pend.append((b - 1, exchange(o_prev)))
            q, k, v, vc, ss = qkv_call(hs[b], wq, wk, wv, vc, b, n_batch)
            s1 = lax.ppermute(ss, 'tp', pairs[1])
            pair_ss = ss + s1
            tot = pair_ss + lax.ppermute(pair_ss, 'tp', pairs[2])
            if b == 1:
                wo_rows, q = lax.optimization_barrier((wo_rows, q))
                w2 = lax.ppermute(wo_rows, 'tp', pairs[2])
                ws = [wo_rows, lax.ppermute(wo_rows, 'tp', pairs[1]), w2, lax.ppermute(w2, 'tp', pairs[1])]
            if len(pend) > 1:
                pb, pos = pend.pop(0)
                pos[0], q = lax.optimization_barrier((pos[0], q))
                out = out_call(pos, ws, x_local, out, pb)
                tot, out = lax.optimization_barrier((tot, out))
            qr, kr, kc = rope_call(q, k, tot, qg, kg, ct, st, kc, b, n_batch, width)
            o_prev = attn_call(qr, kr, v)
        pend.append((n_batch - 1, exchange(o_prev)))
        for pb, pos in pend:
            out = out_call(pos, ws, x_local, out, pb)
        shape = (n_batch, seq, cols // HD, HD)
        return (out, kc.reshape(shape), vc.reshape(shape))

    seq_spec = P('dp', 'tp', None)
    head_spec = P('dp', None, 'tp', None)
    col_spec = P(None, 'tp')
    return jax.shard_map(local_block, mesh=mesh, in_specs=(seq_spec, P(None), col_spec, col_spec, col_spec, P('tp'), P('tp'), P('tp', None)), out_specs=(seq_spec, head_spec, head_spec), check_vma=False)
```

```python
import functools
import math

import jax
import jax.numpy as jnp
from jax import lax
from jax.experimental import pallas as pl
from jax.experimental.pallas import tpu as pltpu
from jax.sharding import PartitionSpec as P


HD = 128
LOG2E = math.log2(math.e)
F32 = jnp.float32
BF16 = jnp.bfloat16
VMEM_LIMIT = 60 * 1024 * 1024


def params(*sem):
    return pltpu.CompilerParams(dimension_semantics=sem, vmem_limit_bytes=VMEM_LIMIT)


def cost(flops, nbytes, trans=0):
    return pl.CostEstimate(flops=int(flops), bytes_accessed=int(nbytes), transcendentals=int(trans))


def rope_tables(seq_len):
    half_dim = HD // 2
    inv_freq = 10000.0 ** (-jnp.arange(half_dim, dtype=F32) * (2.0 / HD))
    angles = jnp.arange(seq_len, dtype=F32)[:, None] * inv_freq[None, :]
    c, s = jnp.cos(angles), jnp.sin(angles)
    return jnp.concatenate([c, c], axis=1), jnp.concatenate([-s, s], axis=1)


def sq_sum(a):
    part = None
    for g in range(a.shape[1] // HD):
        t = a[:, g * HD:(g + 1) * HD]
        part = t * t if part is None else part + t * t
    return jnp.sum(part.T, axis=0, keepdims=True)


def spread_heads(scr, blocks):
    n = len(blocks)
    rows = blocks[0].shape[0]
    for g, t in enumerate(blocks):
        scr[pl.ds(g, rows, stride=n), :] = t
    return scr[...].astype(BF16)


def qkv_kernel(me_ref, ha_ref, hb_ref, wq_ref, wk_ref, wv_ref, *refs):
    q_ref, k_ref, vt_ref, vc_ref, ss_ref, scr = refs[-6:]
    h = jnp.where(pl.program_id(0) == 0, ha_ref[...], hb_ref[...])
    cols = wq_ref.shape[1]
    q = jnp.dot(h, wq_ref[...], preferred_element_type=F32).astype(BF16)
    q_ref[...] = q
    k = jnp.dot(h, wk_ref[...], preferred_element_type=F32).astype(BF16)
    k_ref[...] = k
    ss_ref[0:1, :] = sq_sum(q.astype(F32))
    v = jnp.dot(h, wv_ref[...], preferred_element_type=F32)
    ss_ref[1:2, :] = sq_sum(k.astype(F32))
    vt_ref[...] = v.T.astype(BF16)
    vc_ref[...] = spread_heads(scr, [v[:, g * HD:(g + 1) * HD] for g in range(cols // HD)])


def qkv_call(me, ha, hb, ws, r0, bufs, vc_prev, b, n_batch, seq):
    rows, width = ha.shape
    cols = ws[0].shape[1]
    heads = cols // HD
    bq = 512
    nq = rows // bq
    base = b * (seq // bq)

    def pos(c, i, m):
        return (m[0] ^ (r0 + c)) * nq + i

    wspec = pl.BlockSpec((width, cols), lambda c, i, m: (0, 0))
    rspec = pl.BlockSpec((bq, cols), lambda c, i, m: (pos(c, i, m), 0))
    in_specs = [
        pl.BlockSpec((bq, width), lambda c, i, m: (jnp.where(c == 0, i, nq - 1), 0)),
        pl.BlockSpec((bq, width), lambda c, i, m: (jnp.where(c == 0, 0, i), 0)),
        wspec, wspec, wspec,
    ]
    args = [me, ha, hb, *ws]
    aliases = {}
    for n, buf in enumerate([*(bufs or [None] * 4)[:3], vc_prev, (bufs or [None] * 4)[3]]):
        if buf is not None:
            aliases[len(args)] = n
            args.append(buf)
            in_specs.append(pl.BlockSpec(memory_space=pl.ANY))
    q, k, vt, vc, ss = pl.pallas_call(
        qkv_kernel,
        grid_spec=pltpu.PrefetchScalarGridSpec(
            num_scalar_prefetch=1,
            grid=(2, nq),
            in_specs=in_specs,
            out_specs=[
                rspec, rspec,
                pl.BlockSpec((cols, bq), lambda c, i, m: (0, pos(c, i, m))),
                pl.BlockSpec((bq * heads, HD), lambda c, i, m: (base + pos(c, i, m), 0)),
                pl.BlockSpec((2, bq), lambda c, i, m: (0, pos(c, i, m))),
            ],
            scratch_shapes=[pltpu.VMEM((bq * heads, HD), F32)],
        ),
        out_shape=[
            jax.ShapeDtypeStruct((seq, cols), BF16), jax.ShapeDtypeStruct((seq, cols), BF16), jax.ShapeDtypeStruct((cols, seq), BF16),
            jax.ShapeDtypeStruct((n_batch * seq * heads, HD), BF16), jax.ShapeDtypeStruct((2, seq), F32),
        ],
        input_output_aliases=aliases,
        compiler_params=params("arbitrary", "arbitrary"),
        cost_estimate=cost(12 * rows * width * cols, 4 * rows * width + 6 * width * cols + 16 * rows * cols),
        name="qkv",
    )(*args)
    return [q, k, vt, ss], vc


def rope_kernel(width, q_ref, k_ref, ss_ref, qg_ref, kg_ref, c_ref, s_ref, *refs):
    qr_ref, kr_ref, kc_ref, scr = refs[-4:]
    ct, st = c_ref[...], s_ref[...]
    rows = q_ref.shape[0]
    inv = lax.rsqrt(ss_ref[...] * (1.0 / width) + 1e-5)
    inv_t = jnp.concatenate([inv, jnp.zeros((6, rows), F32)], axis=0).T

    def turn(x_ref, col, g_ref):
        scale = inv_t[:, col:col + 1]
        outs = []
        for g in range(x_ref.shape[1] // HD):
            sl = slice(g * HD, (g + 1) * HD)
            n = x_ref[:, sl].astype(F32) * scale * g_ref[:, sl]
            outs.append(n * ct + pltpu.roll(n, HD // 2, 1) * st)
        return outs

    for g, t in enumerate(turn(q_ref, 0, qg_ref)):
        qr_ref[:, g * HD:(g + 1) * HD] = t.astype(BF16)
    ks = turn(k_ref, 1, kg_ref)
    for g, t in enumerate(ks):
        kr_ref[:, g * HD:(g + 1) * HD] = t.astype(BF16)
    kc_ref[...] = spread_heads(scr, ks)


def rope_call(q, k, ss, qg, kg, ct, st, kc_prev, b, n_batch, width):
    seq, cols = q.shape
    heads = cols // HD
    bq = 512
    nq = seq // bq
    rspec = pl.BlockSpec((bq, cols), lambda i: (i, 0))
    tspec = pl.BlockSpec((bq, HD), lambda i: (i, 0))
    gspec = pl.BlockSpec((1, cols), lambda i: (0, 0))
    in_specs = [rspec, rspec, pl.BlockSpec((2, bq), lambda i: (0, i)), gspec, gspec, tspec, tspec]
    args = [q, k, ss, qg, kg, ct, st]
    aliases = {}
    if kc_prev is not None:
        in_specs.append(pl.BlockSpec(memory_space=pl.ANY))
        args.append(kc_prev)
        aliases = {7: 2}
    base = b * nq
    return pl.pallas_call(
        functools.partial(rope_kernel, width),
        grid=(nq,),
        in_specs=in_specs,
        out_specs=[rspec, rspec, pl.BlockSpec((bq * heads, HD), lambda i: (base + i, 0))],
        out_shape=[jax.ShapeDtypeStruct((seq, cols), BF16)] * 2 + [jax.ShapeDtypeStruct((n_batch * seq * heads, HD), BF16)],
        scratch_shapes=[pltpu.VMEM((bq * heads, HD), F32)],
        input_output_aliases=aliases,
        compiler_params=params("arbitrary"),
        cost_estimate=cost(7e9, 10 * seq * cols),
        name="rope",
    )(*args)


def attn_kernel(n_h, bq, ch, q_ref, k_ref, vt_ref, o_ref, l_s, acc_s, m_s, *stage_refs):
    s_s, mx_s = stage_refs[:n_h], stage_refs[n_h:]
    i = pl.program_id(1)
    c = HD ** -0.5 * LOG2E
    n_c = bq // ch

    def heads(g):
        return slice(g * HD, (g + 1) * HD)

    def span(j, t):
        return pl.ds(pl.multiple_of(j * bq + t * ch, ch), ch)

    def score_chunk(g, j, t, diag, top):
        s = lax.dot_general(k_ref[span(j, t), heads(g)], q_ref[:, heads(g)], (((1,), (1,)), ((), ())), preferred_element_type=F32)
        if diag:
            k_pos = lax.broadcasted_iota(jnp.int32, (ch, bq), 0) + t * ch
            s = jnp.where(lax.broadcasted_iota(jnp.int32, (ch, bq), 1) >= k_pos, s, -1e30)
        s_s[g][t * ch:(t + 1) * ch, :] = s
        part = jnp.max(s.reshape(ch // 8, 8, bq), axis=0)
        return part if top is None else jnp.maximum(top, part)

    def stage(g, j, first, g_next, j_next, diag_next):
        m_new = jnp.max(mx_s[g][...], axis=0, keepdims=True) * c
        if not first:
            m_old = m_s[g]
            m_new = jnp.maximum(m_old, m_new)
            alpha = jnp.exp2(m_old - m_new)
        m_s[g] = m_new
        top = l_new = pv = None
        for t in range(n_c):
            top = score_chunk(g_next, j_next, t, diag_next, top)
            p = jnp.exp2(s_s[g][t * ch:(t + 1) * ch, :] * c - m_new)
            part = jnp.sum(p.reshape(ch // 8, 8, bq), axis=0)
            l_new = part if l_new is None else l_new + part
            part = jnp.dot(vt_ref[heads(g), span(j, t)], p.astype(BF16), preferred_element_type=F32)
            pv = part if pv is None else pv + part
        mx_s[g_next][...] = top
        if first:
            l_s[g] = l_new
            acc_s[g] = pv
        else:
            l_s[g] = l_s[g] * alpha + l_new
            acc_s[g] = acc_s[g] * alpha + pv

    top = None
    for t in range(n_c):
        top = score_chunk(0, i, t, True, top)
    mx_s[0][...] = top
    for g in range(n_h):
        last = g == n_h - 1
        stage(g, i, True, 0 if last else g + 1, 0 if last else i, not last)

    def body(j, carry):
        for g in range(n_h):
            last = g == n_h - 1
            stage(g, j, False, 0 if last else g + 1, jnp.minimum(j + 1, i - 1) if last else j, False)
        return carry

    lax.fori_loop(0, i, body, 0)
    for g in range(n_h):
        l = jnp.sum(l_s[g], axis=0, keepdims=True)
        o_ref[:, heads(g)] = (acc_s[g] / l).T.astype(BF16)


def attn_call(q, k, vt):
    seq, cols = q.shape
    bq, ch, n_h = 512, 256, min(4, cols // HD)
    qspec = pl.BlockSpec((bq, n_h * HD), lambda h, i: (i, h))
    return pl.pallas_call(
        functools.partial(attn_kernel, n_h, bq, ch),
        grid=(cols // (n_h * HD), seq // bq),
        in_specs=[qspec, pl.BlockSpec((seq, n_h * HD), lambda h, i: (0, h)), pl.BlockSpec((n_h * HD, seq), lambda h, i: (h, 0))],
        out_specs=qspec,
        out_shape=jax.ShapeDtypeStruct((seq, cols), BF16),
        scratch_shapes=[pltpu.VMEM((n_h, 8, bq), F32), pltpu.VMEM((n_h, HD, bq), F32), pltpu.VMEM((n_h, 1, bq), F32)]
        + [pltpu.VMEM((bq, bq), F32)] * n_h + [pltpu.VMEM((8, bq), F32)] * n_h,
        compiler_params=params("arbitrary", "arbitrary"),
        cost_estimate=cost(4 * seq * seq * cols, 8 * seq * cols, seq * seq * cols // HD // 2),
        name="attn",
    )(q, k, vt)


def out_kernel(o0, o1, o2, o3, w0, w1, w2, w3, x_ref, *refs):
    out_ref = refs[-1]
    acc = jnp.dot(o0[...], w0[...], preferred_element_type=F32)
    for o, w in ((o1, w1), (o2, w2), (o3, w3)):
        acc += jnp.dot(o[...], w[...], preferred_element_type=F32)
    y = acc.astype(BF16).astype(F32)
    out_ref[0] = (x_ref[0].astype(F32) + y).astype(BF16)


def out_call(os, ws, x, prev, b):
    _, rows, width = x.shape
    cols = os[0].shape[1]
    bn = 512
    ospec = pl.BlockSpec((rows, cols), lambda n: (0, 0))
    wspec = pl.BlockSpec((cols, bn), lambda n: (0, n))
    xspec = pl.BlockSpec((1, rows, bn), lambda n: (b, 0, n))
    in_specs = [ospec] * 4 + [wspec] * 4 + [xspec]
    args = [*os, *ws, x]
    aliases = {}
    if prev is not None:
        in_specs.append(pl.BlockSpec(memory_space=pl.ANY))
        args.append(prev)
        aliases = {9: 0}
    return pl.pallas_call(
        out_kernel,
        grid=(width // bn,),
        in_specs=in_specs,
        out_specs=xspec,
        out_shape=jax.ShapeDtypeStruct(x.shape, BF16),
        input_output_aliases=aliases,
        compiler_params=params("arbitrary"),
        cost_estimate=cost(2 * rows * width * width, 2 * (width * width + 3 * rows * width)),
        name="outproj",
    )(*args)


def solution(mesh):
    n_tp = mesh.shape['tp']
    pairs = {r: [(d, d ^ r) for d in range(n_tp)] for r in range(1, n_tp)}

    def block(x_local, attn_gain, wq, wk, wv, qg, kg, wo_rows):
        n_batch, rows, width = x_local.shape
        seq = rows * n_tp
        cols = wq.shape[1]
        me = lax.axis_index('tp')
        ct, st = rope_tables(seq)

        qg, kg = qg.reshape(1, cols), kg.reshape(1, cols)
        me_arr = me.astype(jnp.int32).reshape(1)
        w_qkv = [wq, wk, wv]

        def after(val, *deps):
            return lax.optimization_barrier((val, *deps))[0]

        def send(val, hop):
            return lax.ppermute(val, 'tp', pairs[hop])

        own = []
        for b in range(n_batch):
            xf = (x_local if b == 0 else after(x_local, own[0]))[b].astype(F32)
            inv_rms = lax.rsqrt(jnp.mean(xf * xf, axis=-1, keepdims=True) + 1e-5)
            own.append((xf * inv_rms * attn_gain).astype(BF16))
        far = [send(own[b], 2) for b in range(2)]
        near = [send(h, 1) for h in own]
        bufs, late, ex, stats = [], [], [], []
        vc = kc = out = ws = None

        def early(b, h1, vc):
            buf, vc = qkv_call(me_arr, own[b], h1, w_qkv, 0, None, vc, b, n_batch, seq)
            bufs.append(buf)
            return vc

        def project(b, vc, *deps):
            h2 = after(far[b], *deps)
            h3 = send(h2, 1)
            buf, vc = qkv_call(me_arr, h2, h3, w_qkv, 2, bufs[b], vc, b, n_batch, seq)
            late.append(buf)
            stats.append(send(buf[3], 2))
            return vc

        def attend(b, kc, *deps):
            q, k, vt, ss = late[b]
            pair_ss = after(stats[b], *deps) + ss
            tot = pair_ss + send(pair_ss, 1)
            qr, kr, kc = rope_call(q, k, tot, qg, kg, ct, st, kc, b, n_batch, width)
            o = attn_call(qr, kr, vt)
            return o, kc

        def exchange(o, *deps):
            pos = []
            for r in range(n_tp):
                piece = lax.dynamic_slice_in_dim(o, (me ^ r) * rows, rows, axis=0)
                pos.append(piece if r == 0 else send(after(piece, *deps), r))
            ex.append(pos)

        for b in range(3):
            vc = early(b, near[b] if b == 0 else after(near[b], vc), vc)
        vc = project(0, vc, vc)
        far.append(send(after(own[2], late[0][3]), 2))
        vc = early(3, after(near[3], vc), vc)
        vc = project(1, vc, vc)
        far.append(send(after(own[3], late[1][3]), 2))
        o0, kc = attend(0, kc, late[1][3])
        vc = project(2, vc, o0)
        w2 = send(after(wo_rows, late[2][3]), 2)
        ws = [wo_rows, send(after(wo_rows, late[2][3]), 1), w2]
        o1, kc = attend(1, kc, late[2][3])
        vc = project(3, vc, o1)
        exchange(o0, late[3][3])
        exchange(o1, late[3][3])
        o2, kc = attend(2, kc, late[3][3])
        exchange(o2)
        ws.append(send(after(w2, o2), 1))
        o3, kc = attend(3, kc, o2)
        exchange(o3)
        for b, pos in enumerate(ex):
            pos[0] = after(pos[0], o3)
            out = out_call(pos, ws, x_local, out, b)
        shape = (n_batch, seq, cols // HD, HD)
        return (out, kc.reshape(shape), vc.reshape(shape))

    seq_spec = P('dp', 'tp', None)
    head_spec = P('dp', None, 'tp', None)
    col_spec = P(None, 'tp')
    return jax.shard_map(block, mesh=mesh, in_specs=(seq_spec, P(None), col_spec, col_spec, col_spec, P('tp'), P('tp'), P('tp', None)), out_specs=(seq_spec, head_spec, head_spec), check_vma=False)
```

```python
import functools
import math

import jax
import jax.numpy as jnp
from jax import lax
from jax.experimental import pallas as pl
from jax.experimental.pallas import tpu as pltpu
from jax.sharding import PartitionSpec as P


HD = 128
LOG2E = math.log2(math.e)
F32 = jnp.float32
BF16 = jnp.bfloat16
QKV_ROWS = 256
VMEM_LIMIT = 60 * 1024 * 1024


def params(*sem):
    return pltpu.CompilerParams(dimension_semantics=sem, vmem_limit_bytes=VMEM_LIMIT)


def cost(flops, nbytes, trans=0):
    return pl.CostEstimate(flops=int(flops), bytes_accessed=int(nbytes), transcendentals=int(trans))


def rope_tables(seq_len):
    half_dim = HD // 2
    inv_freq = 10000.0 ** (-jnp.arange(half_dim, dtype=F32) * (2.0 / HD))
    angles = jnp.arange(seq_len, dtype=F32)[:, None] * inv_freq[None, :]
    c, s = jnp.cos(angles), jnp.sin(angles)
    return jnp.concatenate([c, c], axis=1), jnp.concatenate([-s, s], axis=1)


def sq_sum(a):
    part = None
    for g in range(a.shape[1] // HD):
        t = a[:, g * HD:(g + 1) * HD]
        part = t * t if part is None else part + t * t
    return jnp.sum(part.T, axis=0, keepdims=True)


def spread_heads(scr, blocks):
    n = len(blocks)
    rows = blocks[0].shape[0]
    for g, t in enumerate(blocks):
        scr[pl.ds(g, rows, stride=n), :] = t
    return scr[...].astype(BF16)


def qkv_kernel(n_sub, me_ref, h0_ref, h1_ref, h2_ref, h3_ref, wq_ref, wk_ref, wv_ref, *refs):
    q_ref, k_ref, vt_ref, vc_ref, ss_ref, scr, h_ref = refs[-7:]
    step = pl.program_id(0)
    for n, src in enumerate((h0_ref, h1_ref, h2_ref, h3_ref)):
        @pl.when(step // n_sub == n)
        def _(src=src):
            h_ref[...] = src[...]
    h = h_ref[...]
    cols = wq_ref.shape[1]
    q = jnp.dot(h, wq_ref[...], preferred_element_type=F32).astype(BF16)
    q_ref[...] = q
    k = jnp.dot(h, wk_ref[...], preferred_element_type=F32).astype(BF16)
    k_ref[...] = k
    ss_ref[0:1, :] = sq_sum(q.astype(F32))
    v = jnp.dot(h, wv_ref[...], preferred_element_type=F32)
    ss_ref[1:2, :] = sq_sum(k.astype(F32))
    vt_ref[...] = v.T.astype(BF16)
    vc_ref[...] = spread_heads(scr, [v[:, g * HD:(g + 1) * HD] for g in range(cols // HD)])


def qkv_call(me, hs, ws, r0, bufs, vc_prev, b, n_batch, seq):
    part, width = hs[0].shape
    cols = ws[0].shape[1]
    heads = cols // HD
    bq = QKV_ROWS
    n_sub = part // bq
    base = b * (seq // bq)

    def pos(s, m):
        return (m[0] ^ (r0 + s // (2 * n_sub))) * (2 * n_sub) + s % (2 * n_sub)

    def hspec(n):
        return pl.BlockSpec((bq, width), lambda s, m: (jnp.clip(s - n * n_sub, 0, n_sub - 1), 0))

    wspec = pl.BlockSpec((width, cols), lambda s, m: (0, 0))
    rspec = pl.BlockSpec((bq, cols), lambda s, m: (pos(s, m), 0))
    in_specs = [hspec(n) for n in range(4)] + [wspec, wspec, wspec]
    args = [me, *hs, *ws]
    aliases = {}
    for n, buf in enumerate([*(bufs or [None] * 4)[:3], vc_prev, (bufs or [None] * 4)[3]]):
        if buf is not None:
            aliases[len(args)] = n
            args.append(buf)
            in_specs.append(pl.BlockSpec(memory_space=pl.ANY))
    q, k, vt, vc, ss = pl.pallas_call(
        functools.partial(qkv_kernel, n_sub),
        grid_spec=pltpu.PrefetchScalarGridSpec(
            num_scalar_prefetch=1,
            grid=(4 * n_sub,),
            in_specs=in_specs,
            out_specs=[
                rspec, rspec,
                pl.BlockSpec((cols, bq), lambda s, m: (0, pos(s, m))),
                pl.BlockSpec((bq * heads, HD), lambda s, m: (base + pos(s, m), 0)),
                pl.BlockSpec((2, bq), lambda s, m: (0, pos(s, m))),
            ],
            scratch_shapes=[pltpu.VMEM((bq * heads, HD), F32), pltpu.VMEM((bq, width), BF16)],
        ),
        out_shape=[
            jax.ShapeDtypeStruct((seq, cols), BF16), jax.ShapeDtypeStruct((seq, cols), BF16), jax.ShapeDtypeStruct((cols, seq), BF16),
            jax.ShapeDtypeStruct((n_batch * seq * heads, HD), BF16), jax.ShapeDtypeStruct((2, seq), F32),
        ],
        input_output_aliases=aliases,
        compiler_params=params("arbitrary"),
        cost_estimate=cost(24 * part * width * cols, 8 * part * width + 6 * width * cols + 32 * part * cols),
        name="qkv",
    )(*args)
    return [q, k, vt, ss], vc


def rope_kernel(width, q_ref, k_ref, ss_ref, qg_ref, kg_ref, c_ref, s_ref, *refs):
    qr_ref, kr_ref, kc_ref, scr = refs[-4:]
    ct, st = c_ref[...], s_ref[...]
    rows = q_ref.shape[0]
    inv = lax.rsqrt(ss_ref[...] * (1.0 / width) + 1e-5)
    inv_t = jnp.concatenate([inv, jnp.zeros((6, rows), F32)], axis=0).T

    def turn(x_ref, col, g_ref):
        scale = inv_t[:, col:col + 1]
        outs = []
        for g in range(x_ref.shape[1] // HD):
            sl = slice(g * HD, (g + 1) * HD)
            n = x_ref[:, sl].astype(F32) * scale * g_ref[:, sl]
            outs.append(n * ct + pltpu.roll(n, HD // 2, 1) * st)
        return outs

    for g, t in enumerate(turn(q_ref, 0, qg_ref)):
        qr_ref[:, g * HD:(g + 1) * HD] = t.astype(BF16)
    ks = turn(k_ref, 1, kg_ref)
    for g, t in enumerate(ks):
        kr_ref[:, g * HD:(g + 1) * HD] = t.astype(BF16)
    kc_ref[...] = spread_heads(scr, ks)


def rope_call(q, k, ss, qg, kg, ct, st, kc_prev, b, n_batch, width):
    seq, cols = q.shape
    heads = cols // HD
    bq = 512
    nq = seq // bq
    rspec = pl.BlockSpec((bq, cols), lambda i: (i, 0))
    tspec = pl.BlockSpec((bq, HD), lambda i: (i, 0))
    gspec = pl.BlockSpec((1, cols), lambda i: (0, 0))
    in_specs = [rspec, rspec, pl.BlockSpec((2, bq), lambda i: (0, i)), gspec, gspec, tspec, tspec]
    args = [q, k, ss, qg, kg, ct, st]
    aliases = {}
    if kc_prev is not None:
        in_specs.append(pl.BlockSpec(memory_space=pl.ANY))
        args.append(kc_prev)
        aliases = {7: 2}
    base = b * nq
    return pl.pallas_call(
        functools.partial(rope_kernel, width),
        grid=(nq,),
        in_specs=in_specs,
        out_specs=[rspec, rspec, pl.BlockSpec((bq * heads, HD), lambda i: (base + i, 0))],
        out_shape=[jax.ShapeDtypeStruct((seq, cols), BF16)] * 2 + [jax.ShapeDtypeStruct((n_batch * seq * heads, HD), BF16)],
        scratch_shapes=[pltpu.VMEM((bq * heads, HD), F32)],
        input_output_aliases=aliases,
        compiler_params=params("arbitrary"),
        cost_estimate=cost(7e9, 10 * seq * cols),
        name="rope",
    )(*args)


def attn_kernel(n_h, bq, ch, q_ref, k_ref, vt_ref, o_ref, l_s, acc_s, m_s, *stage_refs):
    s_s, mx_s = stage_refs[:n_h], stage_refs[n_h:]
    i = pl.program_id(1)
    c = HD ** -0.5 * LOG2E
    n_c = bq // ch

    def heads(g):
        return slice(g * HD, (g + 1) * HD)

    def span(j, t):
        return pl.ds(pl.multiple_of(j * bq + t * ch, ch), ch)

    def score_chunk(g, j, t, diag, top):
        s = lax.dot_general(k_ref[span(j, t), heads(g)], q_ref[:, heads(g)], (((1,), (1,)), ((), ())), preferred_element_type=F32)
        if diag:
            k_pos = lax.broadcasted_iota(jnp.int32, (ch, bq), 0) + t * ch
            s = jnp.where(lax.broadcasted_iota(jnp.int32, (ch, bq), 1) >= k_pos, s, -1e30)
        s_s[g][t * ch:(t + 1) * ch, :] = s
        part = jnp.max(s.reshape(ch // 8, 8, bq), axis=0)
        return part if top is None else jnp.maximum(top, part)

    def stage(g, j, first, g_next, j_next, diag_next):
        m_new = jnp.max(mx_s[g][...], axis=0, keepdims=True) * c
        if not first:
            m_old = m_s[g]
            m_new = jnp.maximum(m_old, m_new)
            alpha = jnp.exp2(m_old - m_new)
        m_s[g] = m_new
        top = l_new = pv = None
        for t in range(n_c):
            top = score_chunk(g_next, j_next, t, diag_next, top)
            p = jnp.exp2(s_s[g][t * ch:(t + 1) * ch, :] * c - m_new)
            part = jnp.sum(p.reshape(ch // 8, 8, bq), axis=0)
            l_new = part if l_new is None else l_new + part
            part = jnp.dot(vt_ref[heads(g), span(j, t)], p.astype(BF16), preferred_element_type=F32)
            pv = part if pv is None else pv + part
        mx_s[g_next][...] = top
        if first:
            l_s[g] = l_new
            acc_s[g] = pv
        else:
            l_s[g] = l_s[g] * alpha + l_new
            acc_s[g] = acc_s[g] * alpha + pv

    top = None
    for t in range(n_c):
        top = score_chunk(0, i, t, True, top)
    mx_s[0][...] = top
    for g in range(n_h):
        last = g == n_h - 1
        stage(g, i, True, 0 if last else g + 1, 0 if last else i, not last)

    def body(j, carry):
        for g in range(n_h):
            last = g == n_h - 1
            stage(g, j, False, 0 if last else g + 1, jnp.minimum(j + 1, i - 1) if last else j, False)
        return carry

    lax.fori_loop(0, i, body, 0)
    for g in range(n_h):
        l = jnp.sum(l_s[g], axis=0, keepdims=True)
        o_ref[:, heads(g)] = (acc_s[g] / l).T.astype(BF16)


def attn_call(q, k, vt):
    seq, cols = q.shape
    bq, ch, n_h = 512, 256, min(4, cols // HD)
    qspec = pl.BlockSpec((bq, n_h * HD), lambda h, i: (i, h))
    return pl.pallas_call(
        functools.partial(attn_kernel, n_h, bq, ch),
        grid=(cols // (n_h * HD), seq // bq),
        in_specs=[qspec, pl.BlockSpec((seq, n_h * HD), lambda h, i: (0, h)), pl.BlockSpec((n_h * HD, seq), lambda h, i: (h, 0))],
        out_specs=qspec,
        out_shape=jax.ShapeDtypeStruct((seq, cols), BF16),
        scratch_shapes=[pltpu.VMEM((n_h, 8, bq), F32), pltpu.VMEM((n_h, HD, bq), F32), pltpu.VMEM((n_h, 1, bq), F32)]
        + [pltpu.VMEM((bq, bq), F32)] * n_h + [pltpu.VMEM((8, bq), F32)] * n_h,
        compiler_params=params("arbitrary", "arbitrary"),
        cost_estimate=cost(4 * seq * seq * cols, 8 * seq * cols, seq * seq * cols // HD // 2),
        name="attn",
    )(q, k, vt)


def out_kernel(o0, o1, o2, o3, w0, w1, w2, w3, x_ref, *refs):
    out_ref = refs[-1]
    acc = jnp.dot(o0[...], w0[...], preferred_element_type=F32)
    for o, w in ((o1, w1), (o2, w2), (o3, w3)):
        acc += jnp.dot(o[...], w[...], preferred_element_type=F32)
    y = acc.astype(BF16).astype(F32)
    out_ref[0] = (x_ref[0].astype(F32) + y).astype(BF16)


def out_call(os, ws, x, prev, b):
    _, rows, width = x.shape
    cols = os[0].shape[1]
    bn = 512
    ospec = pl.BlockSpec((rows, cols), lambda n: (0, 0))
    wspec = pl.BlockSpec((cols, bn), lambda n: (0, n))
    xspec = pl.BlockSpec((1, rows, bn), lambda n: (b, 0, n))
    in_specs = [ospec] * 4 + [wspec] * 4 + [xspec]
    args = [*os, *ws, x]
    aliases = {}
    if prev is not None:
        in_specs.append(pl.BlockSpec(memory_space=pl.ANY))
        args.append(prev)
        aliases = {9: 0}
    return pl.pallas_call(
        out_kernel,
        grid=(width // bn,),
        in_specs=in_specs,
        out_specs=xspec,
        out_shape=jax.ShapeDtypeStruct(x.shape, BF16),
        input_output_aliases=aliases,
        compiler_params=params("arbitrary"),
        cost_estimate=cost(2 * rows * width * width, 2 * (width * width + 3 * rows * width)),
        name="outproj",
    )(*args)


def solution(mesh):
    n_tp = mesh.shape['tp']
    pairs = {r: [(d, d ^ r) for d in range(n_tp)] for r in range(1, n_tp)}

    def block(x_local, attn_gain, wq, wk, wv, qg, kg, wo_rows):
        n_batch, rows, width = x_local.shape
        seq = rows * n_tp
        cols = wq.shape[1]
        me = lax.axis_index('tp')
        ct, st = rope_tables(seq)

        qg, kg = qg.reshape(1, cols), kg.reshape(1, cols)
        me_arr = me.astype(jnp.int32).reshape(1)
        w_qkv = [wq, wk, wv]

        def after(val, *deps):
            return lax.optimization_barrier((val, *deps))[0]

        def send(val, hop):
            return lax.ppermute(val, 'tp', pairs[hop])

        half = rows // 2
        own = []
        for b in range(n_batch):
            xs = x_local if b == 0 else after(x_local, own[0][0])
            parts = []
            for p in range(2):
                xf = xs[b, p * half:(p + 1) * half].astype(F32)
                inv_rms = lax.rsqrt(jnp.mean(xf * xf, axis=-1, keepdims=True) + 1e-5)
                parts.append((xf * inv_rms * attn_gain).astype(BF16))
            own.append(parts)
        far = [[None, None] for _ in own]

        def push(b, p, *deps):
            far[b][p] = send(after(own[b][p], *deps) if deps else own[b][p], 2)

        push(0, 0)
        push(0, 1)
        push(1, 0)
        near = [[send(h, 1) for h in parts] for parts in own]
        bufs, late, ex, stats = [], [], [], []
        vc = kc = out = ws = None

        def early(b, vc, *deps):
            n0 = after(near[b][0], *deps) if deps else near[b][0]
            buf, vc = qkv_call(me_arr, [*own[b], n0, near[b][1]], w_qkv, 0, None, vc, b, n_batch, seq)
            bufs.append(buf)
            return vc

        def project(b, vc, *deps):
            h30 = send(far[b][0], 1)
            f1 = after(far[b][1], *deps)
            h31 = send(f1, 1)
            buf, vc = qkv_call(me_arr, [far[b][0], f1, h30, h31], w_qkv, 2, bufs[b], vc, b, n_batch, seq)
            late.append(buf)
            stats.append(send(buf[3], 2))
            return vc

        def attend(b, kc, *deps):
            q, k, vt, ss = late[b]
            pair_ss = after(stats[b], *deps) + ss
            tot = pair_ss + send(pair_ss, 1)
            qr, kr, kc = rope_call(q, k, tot, qg, kg, ct, st, kc, b, n_batch, width)
            o = attn_call(qr, kr, vt)
            return o, kc

        def cut(o, r):
            return lax.dynamic_slice_in_dim(o, (me ^ r) * rows, rows, axis=0)

        def exchange(o, dep):
            o = after(o, dep)
            pieces = [cut(o, r) for r in range(n_tp)]
            return [pieces[0]] + [send(pieces[r], r) for r in range(1, n_tp)]

        vc = early(0, None)
        vc = early(1, vc, vc, ct, st)
        vc = early(2, vc, vc)
        vc = project(0, vc, vc)
        done = late[0][3]
        push(1, 1, done)
        push(2, 0, done)
        vc = early(3, vc, done)
        o0, kc = attend(0, kc, vc)
        pos0 = [cut(o0, r) for r in range(3)]
        pos0 = [pos0[0], send(pos0[1], 1), send(pos0[2], 2)]
        vc = project(1, vc, o0)
        done = late[1][3]
        push(2, 1, done)
        push(3, 0, done)
        piece = cut(after(o0, done), 3)
        ex.append(pos0 + [send(piece, 3)])
        o1, kc = attend(1, kc, piece)
        vc = project(2, vc, o1)
        done = late[2][3]
        push(3, 1, done)
        ex.append(exchange(o1, done))
        o2, kc = attend(2, kc, ex[1][0])
        vc = project(3, vc, o2)
        done = late[3][3]
        wo_late = after(wo_rows, done)
        w2 = send(wo_late, 2)
        ws = [wo_rows, send(wo_late, 1), w2]
        ex.append(exchange(o2, done))
        o3, kc = attend(3, kc, ex[2][0])
        ws.append(send(after(w2, o3), 1))
        ex.append(exchange(o3, o3))
        for b, pos in enumerate(ex):
            pos = [after(pos[0], o3), *pos[1:]]
            out = out_call(pos, ws, x_local, out, b)
        shape = (n_batch, seq, cols // HD, HD)
        return (out, kc.reshape(shape), vc.reshape(shape))

    seq_spec = P('dp', 'tp', None)
    head_spec = P('dp', None, 'tp', None)
    col_spec = P(None, 'tp')
    return jax.shard_map(block, mesh=mesh, in_specs=(seq_spec, P(None), col_spec, col_spec, col_spec, P('tp'), P('tp'), P('tp', None)), out_specs=(seq_spec, head_spec, head_spec), check_vma=False)
```

```python
import functools
import math

import jax
import jax.numpy as jnp
from jax import lax
from jax.experimental import pallas as pl
from jax.experimental.pallas import tpu as pltpu
from jax.sharding import PartitionSpec as P


HD = 128
LOG2E = math.log2(math.e)
F32 = jnp.float32
BF16 = jnp.bfloat16
QKV_ROWS = 256
VMEM_LIMIT = 60 * 1024 * 1024


def params(*sem):
    return pltpu.CompilerParams(dimension_semantics=sem, vmem_limit_bytes=VMEM_LIMIT)


def cost(flops, nbytes, trans=0):
    return pl.CostEstimate(flops=int(flops), bytes_accessed=int(nbytes), transcendentals=int(trans))


def rope_tables(seq_len):
    fine = 64
    lane = jnp.arange(HD)
    inv_freq = 10000.0 ** (-(lane % (HD // 2)).astype(F32) * (2.0 / HD))
    low = jnp.arange(fine, dtype=F32)[:, None] * inv_freq[None, :]
    high = (jnp.arange(seq_len // fine) * fine).astype(F32)[:, None] * inv_freq[None, :]
    cl, sl, ch, sh = lax.optimization_barrier((jnp.cos(low)[None], jnp.sin(low)[None], jnp.cos(high)[:, None], jnp.sin(high)[:, None]))
    c = (ch * cl - sh * sl).reshape(seq_len, HD)
    s = (sh * cl + ch * sl).reshape(seq_len, HD)
    return c, jnp.where(lane < HD // 2, -s, s)


def sq_sum(a):
    part = None
    for g in range(a.shape[1] // HD):
        t = a[:, g * HD:(g + 1) * HD]
        part = t * t if part is None else part + t * t
    return jnp.sum(part.T, axis=0, keepdims=True)


def spread_heads(scr, blocks):
    n = len(blocks)
    rows = blocks[0].shape[0]
    for g, t in enumerate(blocks):
        scr[pl.ds(g, rows, stride=n), :] = t
    return scr[...].astype(BF16)


def norm_kernel(x_ref, g_ref, a_ref, b_ref):
    x = x_ref[0].astype(F32)
    mean = jnp.sum(x * x, axis=1, keepdims=True) * (1.0 / x.shape[1])
    h = (x * lax.rsqrt(mean + 1e-5) * g_ref[...]).astype(BF16)
    lower = pl.program_id(0) < pl.num_programs(0) // 2

    @pl.when(lower)
    def _():
        a_ref[...] = h

    @pl.when(jnp.logical_not(lower))
    def _():
        b_ref[...] = h


def norm_call(x, gain, b):
    rows, width = x.shape[1:]
    br = 256
    n = rows // br
    half = jax.ShapeDtypeStruct((rows // 2, width), BF16)
    return pl.pallas_call(
        norm_kernel,
        grid=(n,),
        in_specs=[pl.BlockSpec((1, br, width), lambda s: (b, s, 0)), pl.BlockSpec((1, width), lambda s: (0, 0))],
        out_specs=[pl.BlockSpec((br, width), lambda s: (jnp.minimum(s, n // 2 - 1), 0)), pl.BlockSpec((br, width), lambda s: (jnp.maximum(s - n // 2, 0), 0))],
        out_shape=[half, half],
        compiler_params=params("arbitrary"),
        cost_estimate=cost(8 * rows * width, 4 * rows * width),
        name="norm",
    )(x, gain)


def qkv_kernel(n_sub, me_ref, h0_ref, h1_ref, h2_ref, h3_ref, wq_ref, wk_ref, wv_ref, *refs):
    q_ref, k_ref, vt_ref, vc_ref, ss_ref, scr, h_ref = refs[-7:]
    step = pl.program_id(0)
    for n, src in enumerate((h0_ref, h1_ref, h2_ref, h3_ref)):
        @pl.when(step // n_sub == n)
        def _(src=src):
            h_ref[...] = src[...]
    h = h_ref[...]
    cols = wq_ref.shape[1]
    q = jnp.dot(h, wq_ref[...], preferred_element_type=F32).astype(BF16)
    q_ref[...] = q
    k = jnp.dot(h, wk_ref[...], preferred_element_type=F32).astype(BF16)
    k_ref[...] = k
    ss_ref[0:1, :] = sq_sum(q.astype(F32))
    v = jnp.dot(h, wv_ref[...], preferred_element_type=F32)
    ss_ref[1:2, :] = sq_sum(k.astype(F32))
    vt_ref[...] = v.T.astype(BF16)
    vc_ref[...] = spread_heads(scr, [v[:, g * HD:(g + 1) * HD] for g in range(cols // HD)])


def qkv_call(me, hs, ws, r0, bufs, vc_prev, b, n_batch, seq):
    part, width = hs[0].shape
    cols = ws[0].shape[1]
    heads = cols // HD
    bq = QKV_ROWS
    n_sub = part // bq
    base = b * (seq // bq)

    def pos(s, m):
        return (m[0] ^ (r0 + s // (2 * n_sub))) * (2 * n_sub) + s % (2 * n_sub)

    def hspec(n):
        return pl.BlockSpec((bq, width), lambda s, m: (jnp.clip(s - n * n_sub, 0, n_sub - 1), 0))

    wspec = pl.BlockSpec((width, cols), lambda s, m: (0, 0))
    rspec = pl.BlockSpec((bq, cols), lambda s, m: (pos(s, m), 0))
    in_specs = [hspec(n) for n in range(4)] + [wspec, wspec, wspec]
    args = [me, *hs, *ws]
    aliases = {}
    for n, buf in enumerate([*(bufs or [None] * 4)[:3], vc_prev, (bufs or [None] * 4)[3]]):
        if buf is not None:
            aliases[len(args)] = n
            args.append(buf)
            in_specs.append(pl.BlockSpec(memory_space=pl.ANY))
    q, k, vt, vc, ss = pl.pallas_call(
        functools.partial(qkv_kernel, n_sub),
        grid_spec=pltpu.PrefetchScalarGridSpec(
            num_scalar_prefetch=1,
            grid=(4 * n_sub,),
            in_specs=in_specs,
            out_specs=[
                rspec, rspec,
                pl.BlockSpec((cols, bq), lambda s, m: (0, pos(s, m))),
                pl.BlockSpec((bq * heads, HD), lambda s, m: (base + pos(s, m), 0)),
                pl.BlockSpec((2, bq), lambda s, m: (0, pos(s, m))),
            ],
            scratch_shapes=[pltpu.VMEM((bq * heads, HD), F32), pltpu.VMEM((bq, width), BF16)],
        ),
        out_shape=[
            jax.ShapeDtypeStruct((seq, cols), BF16), jax.ShapeDtypeStruct((seq, cols), BF16), jax.ShapeDtypeStruct((cols, seq), BF16),
            jax.ShapeDtypeStruct((n_batch * seq * heads, HD), BF16), jax.ShapeDtypeStruct((2, seq), F32),
        ],
        input_output_aliases=aliases,
        compiler_params=params("arbitrary"),
        cost_estimate=cost(24 * part * width * cols, 8 * part * width + 6 * width * cols + 32 * part * cols),
        name="qkv",
    )(*args)
    return [q, k, vt, ss], vc


def rope_kernel(width, q_ref, k_ref, ss_ref, qg_ref, kg_ref, c_ref, s_ref, *refs):
    qr_ref, kr_ref, kc_ref, scr = refs[-4:]
    ct, st = c_ref[...], s_ref[...]
    rows = q_ref.shape[0]
    inv = lax.rsqrt(ss_ref[...] * (1.0 / width) + 1e-5)
    inv_t = jnp.concatenate([inv, jnp.zeros((6, rows), F32)], axis=0).T

    def turn(x_ref, col, g_ref):
        scale = inv_t[:, col:col + 1]
        outs = []
        for g in range(x_ref.shape[1] // HD):
            sl = slice(g * HD, (g + 1) * HD)
            n = x_ref[:, sl].astype(F32) * scale * g_ref[:, sl]
            outs.append(n * ct + pltpu.roll(n, HD // 2, 1) * st)
        return outs

    for g, t in enumerate(turn(q_ref, 0, qg_ref)):
        qr_ref[:, g * HD:(g + 1) * HD] = t.astype(BF16)
    ks = turn(k_ref, 1, kg_ref)
    for g, t in enumerate(ks):
        kr_ref[:, g * HD:(g + 1) * HD] = t.astype(BF16)
    kc_ref[...] = spread_heads(scr, ks)


def rope_call(q, k, ss, qg, kg, ct, st, kc_prev, b, n_batch, width):
    seq, cols = q.shape
    heads = cols // HD
    bq = 512
    nq = seq // bq
    rspec = pl.BlockSpec((bq, cols), lambda i: (i, 0))
    tspec = pl.BlockSpec((bq, HD), lambda i: (i, 0))
    gspec = pl.BlockSpec((1, cols), lambda i: (0, 0))
    in_specs = [rspec, rspec, pl.BlockSpec((2, bq), lambda i: (0, i)), gspec, gspec, tspec, tspec]
    args = [q, k, ss, qg, kg, ct, st]
    aliases = {}
    if kc_prev is not None:
        in_specs.append(pl.BlockSpec(memory_space=pl.ANY))
        args.append(kc_prev)
        aliases = {7: 2}
    base = b * nq
    return pl.pallas_call(
        functools.partial(rope_kernel, width),
        grid=(nq,),
        in_specs=in_specs,
        out_specs=[rspec, rspec, pl.BlockSpec((bq * heads, HD), lambda i: (base + i, 0))],
        out_shape=[jax.ShapeDtypeStruct((seq, cols), BF16)] * 2 + [jax.ShapeDtypeStruct((n_batch * seq * heads, HD), BF16)],
        scratch_shapes=[pltpu.VMEM((bq * heads, HD), F32)],
        input_output_aliases=aliases,
        compiler_params=params("arbitrary"),
        cost_estimate=cost(7e9, 10 * seq * cols),
        name="rope",
    )(*args)


def attn_kernel(n_h, bq, ch, q_ref, k_ref, vt_ref, o_ref, l_s, acc_s, m_s, *stage_refs):
    s_s, mx_s = stage_refs[:n_h], stage_refs[n_h:]
    i = pl.program_id(1)
    c = HD ** -0.5 * LOG2E
    n_c = bq // ch

    def heads(g):
        return slice(g * HD, (g + 1) * HD)

    def span(j, t):
        return pl.ds(pl.multiple_of(j * bq + t * ch, ch), ch)

    def score_chunk(g, j, t, diag, top):
        s = lax.dot_general(k_ref[span(j, t), heads(g)], q_ref[:, heads(g)], (((1,), (1,)), ((), ())), preferred_element_type=F32)
        if diag:
            k_pos = lax.broadcasted_iota(jnp.int32, (ch, bq), 0) + t * ch
            s = jnp.where(lax.broadcasted_iota(jnp.int32, (ch, bq), 1) >= k_pos, s, -1e30)
        s_s[g][t * ch:(t + 1) * ch, :] = s
        part = jnp.max(s.reshape(ch // 8, 8, bq), axis=0)
        return part if top is None else jnp.maximum(top, part)

    def stage(g, j, first, g_next, j_next, diag_next):
        m_new = jnp.max(mx_s[g][...], axis=0, keepdims=True) * c
        if not first:
            m_old = m_s[g]
            m_new = jnp.maximum(m_old, m_new)
            alpha = jnp.exp2(m_old - m_new)
        m_s[g] = m_new
        top = l_new = pv = None
        for t in range(n_c):
            top = score_chunk(g_next, j_next, t, diag_next, top)
            p = jnp.exp2(s_s[g][t * ch:(t + 1) * ch, :] * c - m_new)
            part = jnp.sum(p.reshape(ch // 8, 8, bq), axis=0)
            l_new = part if l_new is None else l_new + part
            part = jnp.dot(vt_ref[heads(g), span(j, t)], p.astype(BF16), preferred_element_type=F32)
            pv = part if pv is None else pv + part
        mx_s[g_next][...] = top
        if first:
            l_s[g] = l_new
            acc_s[g] = pv
        else:
            l_s[g] = l_s[g] * alpha + l_new
            acc_s[g] = acc_s[g] * alpha + pv

    top = None
    for t in range(n_c):
        top = score_chunk(0, i, t, True, top)
    mx_s[0][...] = top
    for g in range(n_h):
        last = g == n_h - 1
        stage(g, i, True, 0 if last else g + 1, 0 if last else i, not last)

    def body(j, carry):
        for g in range(n_h):
            last = g == n_h - 1
            stage(g, j, False, 0 if last else g + 1, jnp.minimum(j + 1, i - 1) if last else j, False)
        return carry

    lax.fori_loop(0, i, body, 0)
    for g in range(n_h):
        l = jnp.sum(l_s[g], axis=0, keepdims=True)
        o_ref[:, heads(g)] = (acc_s[g] / l).T.astype(BF16)


def attn_call(q, k, vt):
    seq, cols = q.shape
    bq, ch, n_h = 512, 256, min(4, cols // HD)
    qspec = pl.BlockSpec((bq, n_h * HD), lambda h, i: (i, h))
    return pl.pallas_call(
        functools.partial(attn_kernel, n_h, bq, ch),
        grid=(cols // (n_h * HD), seq // bq),
        in_specs=[qspec, pl.BlockSpec((seq, n_h * HD), lambda h, i: (0, h)), pl.BlockSpec((n_h * HD, seq), lambda h, i: (h, 0))],
        out_specs=qspec,
        out_shape=jax.ShapeDtypeStruct((seq, cols), BF16),
        scratch_shapes=[pltpu.VMEM((n_h, 8, bq), F32), pltpu.VMEM((n_h, HD, bq), F32), pltpu.VMEM((n_h, 1, bq), F32)]
        + [pltpu.VMEM((bq, bq), F32)] * n_h + [pltpu.VMEM((8, bq), F32)] * n_h,
        compiler_params=params("arbitrary", "arbitrary"),
        cost_estimate=cost(4 * seq * seq * cols, 8 * seq * cols, seq * seq * cols // HD // 2),
        name="attn",
    )(q, k, vt)


def out_kernel(n_items, *refs):
    pieces, (w0, w1, w2, w3, x_ref) = refs[:4 * n_items], refs[4 * n_items:4 * n_items + 5]
    out_ref, o_buf, sems = refs[-3:]
    item, n = pl.program_id(0), pl.program_id(1)

    def loads(t):
        return [pltpu.make_async_copy(pieces[4 * t + r], o_buf.at[t % 2, r], sems.at[t % 2, r]) for r in range(4)]

    for t in range(n_items):
        @pl.when((item == max(t - 1, 0)) & (n == (1 if t else 0)))
        def _(t=t):
            for load in loads(t):
                load.start()

        @pl.when((item == t) & (n == 0))
        def _(t=t):
            for load in loads(t):
                load.wait()

    slot = item % 2
    acc = jnp.dot(o_buf[slot, 0], w0[...], preferred_element_type=F32)
    for r, w in ((1, w1), (2, w2), (3, w3)):
        acc += jnp.dot(o_buf[slot, r], w[...], preferred_element_type=F32)
    y = acc.astype(BF16).astype(F32)
    out_ref[0] = (x_ref[0].astype(F32) + y).astype(BF16)


def out_call(items, ws, x, prev, b, part):
    width = x.shape[2]
    n_items = len(items)
    rows, cols = items[0][0].shape
    bn = 512
    hbm = pl.BlockSpec(memory_space=pl.ANY)
    wspec = pl.BlockSpec((cols, bn), lambda t, n: (0, n))
    xspec = pl.BlockSpec((1, rows, bn), lambda t, n: (b + t, part, n))
    in_specs = [hbm] * (4 * n_items) + [wspec] * 4 + [xspec]
    args = [*sum(items, []), *ws, x]
    aliases = {}
    if prev is not None:
        aliases = {len(args): 0}
        in_specs.append(hbm)
        args.append(prev)
    return pl.pallas_call(
        functools.partial(out_kernel, n_items),
        grid=(n_items, width // bn),
        in_specs=in_specs,
        out_specs=xspec,
        out_shape=jax.ShapeDtypeStruct(x.shape, BF16),
        scratch_shapes=[pltpu.VMEM((2, 4, rows, cols), BF16), pltpu.SemaphoreType.DMA((2, 4))],
        input_output_aliases=aliases,
        compiler_params=params("arbitrary", "arbitrary"),
        cost_estimate=cost(2 * n_items * rows * width * width, n_items * (2 * width * width + 6 * rows * width)),
        name="outproj",
    )(*args)


def solution(mesh):
    n_tp = mesh.shape['tp']
    pairs = {r: [(d, d ^ r) for d in range(n_tp)] for r in range(1, n_tp)}

    def block(x_local, attn_gain, wq, wk, wv, qg, kg, wo_rows):
        n_batch, rows, width = x_local.shape
        seq = rows * n_tp
        cols = wq.shape[1]
        me = lax.axis_index('tp')
        ct, st = rope_tables(seq)

        qg, kg = qg.reshape(1, cols), kg.reshape(1, cols)
        me_arr = me.astype(jnp.int32).reshape(1)
        w_qkv = [wq, wk, wv]

        def after(val, *deps):
            return lax.optimization_barrier((val, *deps))[0]

        def send(val, hop):
            return lax.ppermute(val, 'tp', pairs[hop])

        gain = attn_gain.reshape(1, width)
        own = []
        for b in range(n_batch):
            own.append(norm_call(x_local, after(gain, own[-1][0]) if own else gain, b))
        far = [[None, None] for _ in own]

        def push(b, p, *deps):
            far[b][p] = send(after(own[b][p], *deps) if deps else own[b][p], 2)

        push(0, 0)
        push(0, 1)
        push(1, 0)
        near = [[send(h, 1) for h in parts] for parts in own]
        bufs, late, ex, stats = [], [], [], []
        vc = kc = out = ws = None

        def early(b, vc, *deps):
            n0 = after(near[b][0], *deps) if deps else near[b][0]
            buf, vc = qkv_call(me_arr, [*own[b], n0, near[b][1]], w_qkv, 0, None, vc, b, n_batch, seq)
            bufs.append(buf)
            return vc

        def project(b, vc, *deps):
            h30 = send(far[b][0], 1)
            f1 = after(far[b][1], *deps)
            h31 = send(f1, 1)
            buf, vc = qkv_call(me_arr, [far[b][0], f1, h30, h31], w_qkv, 2, bufs[b], vc, b, n_batch, seq)
            late.append(buf)
            stats.append(send(buf[3], 2))
            return vc

        def attend(b, kc, *deps):
            q, k, vt, ss = late[b]
            pair_ss = after(stats[b], *deps) + ss
            tot = pair_ss + send(pair_ss, 1)
            qr, kr, kc = rope_call(q, k, tot, qg, kg, ct, st, kc, b, n_batch, width)
            o = attn_call(qr, kr, vt)
            return o, kc

        def exchange(o, dep, n_parts=1):
            o = after(o, dep)
            size = rows // n_parts
            pieces = [[lax.dynamic_slice_in_dim(o, (me ^ r) * rows + p * size, size, axis=0) for r in range(n_tp)] for p in range(n_parts)]
            return [[cut[0]] + [send(cut[r], r) for r in range(1, n_tp)] for cut in pieces]

        vc = early(0, None)
        vc = early(1, vc, vc, ct, st)
        vc = early(2, vc, vc)
        vc = project(0, vc, vc)
        done = late[0][3]
        push(1, 1, done)
        push(2, 0, done)
        vc = early(3, vc, done)
        w_cut = [0, cols // 2, 3 * cols // 4, cols]

        def push_w(n, dep):
            return send(after(wo_rows, dep)[w_cut[n]:w_cut[n + 1]], 2)

        w2 = [push_w(0, done)]
        o0, kc = attend(0, kc, vc)
        vc = project(1, vc, o0)
        done = late[1][3]
        push(2, 1, done)
        push(3, 0, done)
        w2.append(push_w(1, done))
        ex.append(exchange(o0, done))
        o1, kc = attend(1, kc, ex[0][0][0])
        vc = project(2, vc, o1)
        done = late[2][3]
        push(3, 1, done)
        w2.append(push_w(2, done))
        ex.append(exchange(o1, done))
        o2, kc = attend(2, kc, ex[1][0][0])
        vc = project(3, vc, o2)
        done = late[3][3]
        ex.append(exchange(o2, done))
        o3, kc = attend(3, kc, ex[2][0][0])
        ex.append(exchange(o3, o3, 2))
        w2 = jnp.concatenate([after(w2[0], ex[3][0][0]), *w2[1:]], axis=0)
        ws = [wo_rows, send(after(wo_rows, done), 1), w2, send(w2, 1)]
        first = [list(parts[0]) for parts in ex[:-1]]
        first[0][0] = after(first[0][0], ex[3][0][0])
        out = out_call(first, ws, x_local, None, 0, 0)
        for p, pos in enumerate(ex[-1]):
            out = out_call([pos], ws, x_local, out, n_batch - 1, p)
        shape = (n_batch, seq, cols // HD, HD)
        return (out, kc.reshape(shape), vc.reshape(shape))

    seq_spec = P('dp', 'tp', None)
    head_spec = P('dp', None, 'tp', None)
    col_spec = P(None, 'tp')
    return jax.shard_map(block, mesh=mesh, in_specs=(seq_spec, P(None), col_spec, col_spec, col_spec, P('tp'), P('tp'), P('tp', None)), out_specs=(seq_spec, head_spec, head_spec), check_vma=False)
```

```python
import functools
import math

import jax
import jax.numpy as jnp
from jax import lax
from jax.experimental import pallas as pl
from jax.experimental.pallas import tpu as pltpu
from jax.sharding import PartitionSpec as P


HD = 128
LOG2E = math.log2(math.e)
F32 = jnp.float32
BF16 = jnp.bfloat16
QKV_ROWS = 256
VMEM_LIMIT = 60 * 1024 * 1024


def params(*sem):
    return pltpu.CompilerParams(dimension_semantics=sem, vmem_limit_bytes=VMEM_LIMIT)


def cost(flops, nbytes, trans=0):
    return pl.CostEstimate(flops=int(flops), bytes_accessed=int(nbytes), transcendentals=int(trans))


def rope_tables(seq_len):
    fine = 64
    lane = jnp.arange(HD)
    inv_freq = 10000.0 ** (-(lane % (HD // 2)).astype(F32) * (2.0 / HD))
    low = jnp.arange(fine, dtype=F32)[:, None] * inv_freq[None, :]
    high = (jnp.arange(seq_len // fine) * fine).astype(F32)[:, None] * inv_freq[None, :]
    cl, sl, ch, sh = lax.optimization_barrier((jnp.cos(low)[None], jnp.sin(low)[None], jnp.cos(high)[:, None], jnp.sin(high)[:, None]))
    c = (ch * cl - sh * sl).reshape(seq_len, HD)
    s = (sh * cl + ch * sl).reshape(seq_len, HD)
    return c, jnp.where(lane < HD // 2, -s, s)


def sq_sum(a):
    part = None
    for g in range(a.shape[1] // HD):
        t = a[:, g * HD:(g + 1) * HD]
        part = t * t if part is None else part + t * t
    return jnp.sum(part.T, axis=0, keepdims=True)


def spread_heads(scr, blocks):
    n = len(blocks)
    rows = blocks[0].shape[0]
    for g, t in enumerate(blocks):
        scr[pl.ds(g, rows, stride=n), :] = t
    return scr[...].astype(BF16)


def norm_kernel(x_ref, g_ref, a_ref, b_ref):
    rows, width = a_ref.shape
    lower = pl.program_id(0) < pl.num_programs(0) // 2
    for first, dst in ((True, a_ref), (False, b_ref)):
        @pl.when(lower == first)
        def _(dst=dst):
            @pl.loop(0, rows // 64)
            def _(t):
                part = pl.ds(pl.multiple_of(t * 64, 64), 64)
                x = x_ref[0, part, :].astype(F32)
                mean = jnp.sum(x * x, axis=1, keepdims=True) * (1.0 / width)
                dst[part, :] = (x * lax.rsqrt(mean + 1e-5) * g_ref[...]).astype(BF16)


def norm_call(x, gain, b):
    rows, width = x.shape[1:]
    br = 256
    n = rows // br
    half = jax.ShapeDtypeStruct((rows // 2, width), BF16)
    return pl.pallas_call(
        norm_kernel,
        grid=(n,),
        in_specs=[pl.BlockSpec((1, br, width), lambda s: (b, s, 0)), pl.BlockSpec((1, width), lambda s: (0, 0))],
        out_specs=[pl.BlockSpec((br, width), lambda s: (jnp.minimum(s, n // 2 - 1), 0)), pl.BlockSpec((br, width), lambda s: (jnp.maximum(s - n // 2, 0), 0))],
        out_shape=[half, half],
        compiler_params=params("arbitrary"),
        cost_estimate=cost(8 * rows * width, 4 * rows * width),
        name="norm",
    )(x, gain)


def qkv_kernel(n_sub, me_ref, h0_ref, h1_ref, h2_ref, h3_ref, wq_ref, wk_ref, wv_ref, *refs):
    q_ref, k_ref, vt_ref, vc_ref, ss_ref, scr, h_ref = refs[-7:]
    step = pl.program_id(0)
    for n, src in enumerate((h0_ref, h1_ref, h2_ref, h3_ref)):
        @pl.when(step // n_sub == n)
        def _(src=src):
            @pl.loop(0, src.shape[0] // 64)
            def _(t):
                part = pl.ds(pl.multiple_of(t * 64, 64), 64)
                h_ref[part, :] = src[part, :]
    h = h_ref[...]
    cols = wq_ref.shape[1]
    q = jnp.dot(h, wq_ref[...], preferred_element_type=F32).astype(BF16)
    q_ref[...] = q
    k = jnp.dot(h, wk_ref[...], preferred_element_type=F32).astype(BF16)
    k_ref[...] = k
    ss_ref[0:1, :] = sq_sum(q.astype(F32))
    v = jnp.dot(h, wv_ref[...], preferred_element_type=F32)
    ss_ref[1:2, :] = sq_sum(k.astype(F32))
    vt_ref[...] = v.T.astype(BF16)
    vc_ref[...] = spread_heads(scr, [v[:, g * HD:(g + 1) * HD] for g in range(cols // HD)])


def qkv_call(me, hs, ws, r0, bufs, vc_prev, b, n_batch, seq):
    part, width = hs[0].shape
    cols = ws[0].shape[1]
    heads = cols // HD
    bq = QKV_ROWS
    n_sub = part // bq
    base = b * (seq // bq)

    def pos(s, m):
        return (m[0] ^ (r0 + s // (2 * n_sub))) * (2 * n_sub) + s % (2 * n_sub)

    def hspec(n):
        return pl.BlockSpec((bq, width), lambda s, m: (jnp.clip(s - n * n_sub, 0, n_sub - 1), 0))

    wspec = pl.BlockSpec((width, cols), lambda s, m: (0, 0))
    rspec = pl.BlockSpec((bq, cols), lambda s, m: (pos(s, m), 0))
    in_specs = [hspec(n) for n in range(4)] + [wspec, wspec, wspec]
    args = [me, *hs, *ws]
    aliases = {}
    for n, buf in enumerate([*(bufs or [None] * 4)[:3], vc_prev, (bufs or [None] * 4)[3]]):
        if buf is not None:
            aliases[len(args)] = n
            args.append(buf)
            in_specs.append(pl.BlockSpec(memory_space=pl.ANY))
    q, k, vt, vc, ss = pl.pallas_call(
        functools.partial(qkv_kernel, n_sub),
        grid_spec=pltpu.PrefetchScalarGridSpec(
            num_scalar_prefetch=1,
            grid=(4 * n_sub,),
            in_specs=in_specs,
            out_specs=[
                rspec, rspec,
                pl.BlockSpec((cols, bq), lambda s, m: (0, pos(s, m))),
                pl.BlockSpec((bq * heads, HD), lambda s, m: (base + pos(s, m), 0)),
                pl.BlockSpec((2, bq), lambda s, m: (0, pos(s, m))),
            ],
            scratch_shapes=[pltpu.VMEM((bq * heads, HD), F32), pltpu.VMEM((bq, width), BF16)],
        ),
        out_shape=[
            jax.ShapeDtypeStruct((seq, cols), BF16), jax.ShapeDtypeStruct((seq, cols), BF16), jax.ShapeDtypeStruct((cols, seq), BF16),
            jax.ShapeDtypeStruct((n_batch * seq * heads, HD), BF16), jax.ShapeDtypeStruct((2, seq), F32),
        ],
        input_output_aliases=aliases,
        compiler_params=params("arbitrary"),
        cost_estimate=cost(24 * part * width * cols, 8 * part * width + 6 * width * cols + 32 * part * cols),
        name="qkv",
    )(*args)
    return [q, k, vt, ss], vc


def rope_kernel(width, q_ref, k_ref, ss_ref, qg_ref, kg_ref, c_ref, s_ref, *refs):
    qr_ref, kr_ref, kc_ref, scr = refs[-4:]
    ct, st = c_ref[...], s_ref[...]
    rows = q_ref.shape[0]
    inv = lax.rsqrt(ss_ref[...] * (1.0 / width) + 1e-5)
    inv_t = jnp.concatenate([inv, jnp.zeros((6, rows), F32)], axis=0).T

    def turn(x_ref, col, g_ref):
        scale = inv_t[:, col:col + 1]
        outs = []
        for g in range(x_ref.shape[1] // HD):
            sl = slice(g * HD, (g + 1) * HD)
            n = x_ref[:, sl].astype(F32) * scale * g_ref[:, sl]
            outs.append(n * ct + pltpu.roll(n, HD // 2, 1) * st)
        return outs

    for g, t in enumerate(turn(q_ref, 0, qg_ref)):
        qr_ref[:, g * HD:(g + 1) * HD] = t.astype(BF16)
    ks = turn(k_ref, 1, kg_ref)
    for g, t in enumerate(ks):
        kr_ref[:, g * HD:(g + 1) * HD] = t.astype(BF16)
    kc_ref[...] = spread_heads(scr, ks)


def rope_call(q, k, ss, qg, kg, ct, st, kc_prev, b, n_batch, width):
    seq, cols = q.shape
    heads = cols // HD
    bq = 512
    nq = seq // bq
    rspec = pl.BlockSpec((bq, cols), lambda i: (i, 0))
    tspec = pl.BlockSpec((bq, HD), lambda i: (i, 0))
    gspec = pl.BlockSpec((1, cols), lambda i: (0, 0))
    in_specs = [rspec, rspec, pl.BlockSpec((2, bq), lambda i: (0, i)), gspec, gspec, tspec, tspec]
    args = [q, k, ss, qg, kg, ct, st]
    aliases = {}
    if kc_prev is not None:
        in_specs.append(pl.BlockSpec(memory_space=pl.ANY))
        args.append(kc_prev)
        aliases = {7: 2}
    base = b * nq
    return pl.pallas_call(
        functools.partial(rope_kernel, width),
        grid=(nq,),
        in_specs=in_specs,
        out_specs=[rspec, rspec, pl.BlockSpec((bq * heads, HD), lambda i: (base + i, 0))],
        out_shape=[jax.ShapeDtypeStruct((seq, cols), BF16)] * 2 + [jax.ShapeDtypeStruct((n_batch * seq * heads, HD), BF16)],
        scratch_shapes=[pltpu.VMEM((bq * heads, HD), F32)],
        input_output_aliases=aliases,
        compiler_params=params("arbitrary"),
        cost_estimate=cost(7e9, 10 * seq * cols),
        name="rope",
    )(*args)


def attn_kernel(n_tp, n_parts, n_h, bq, ch, q_ref, k_ref, vt_ref, *refs):
    outs = refs[:n_tp * n_parts]
    l_s, acc_s, m_s, o_s, sem, *stage_refs = refs[n_tp * n_parts:]
    me = lax.axis_index('tp')
    n_q = pl.num_programs(0)
    per = n_q // n_tp
    s_s, mx_s = stage_refs[:n_h], stage_refs[n_h:]
    i = pl.program_id(0)
    c = HD ** -0.5 * LOG2E
    n_c = bq // ch

    def heads(g):
        return slice(g * HD, (g + 1) * HD)

    def span(j, t):
        return pl.ds(pl.multiple_of(j * bq + t * ch, ch), ch)

    def score_chunk(g, j, t, diag, top):
        s = lax.dot_general(k_ref[span(j, t), heads(g)], q_ref[:, heads(g)], (((1,), (1,)), ((), ())), preferred_element_type=F32)
        if diag:
            k_pos = lax.broadcasted_iota(jnp.int32, (ch, bq), 0) + t * ch
            s = jnp.where(lax.broadcasted_iota(jnp.int32, (ch, bq), 1) >= k_pos, s, -1e30)
        s_s[g][t * ch:(t + 1) * ch, :] = s
        part = jnp.max(s.reshape(ch // 8, 8, bq), axis=0)
        return part if top is None else jnp.maximum(top, part)

    def stage(g, j, first, g_next, j_next, diag_next):
        m_new = jnp.max(mx_s[g][...], axis=0, keepdims=True) * c
        if not first:
            m_old = m_s[g]
            m_new = jnp.maximum(m_old, m_new)
            alpha = jnp.exp2(m_old - m_new)
        m_s[g] = m_new
        top = l_new = pv = None
        for t in range(n_c):
            top = score_chunk(g_next, j_next, t, diag_next, top)
            p = jnp.exp2(s_s[g][t * ch:(t + 1) * ch, :] * c - m_new)
            part = jnp.sum(p.reshape(ch // 8, 8, bq), axis=0)
            l_new = part if l_new is None else l_new + part
            part = jnp.dot(vt_ref[heads(g), span(j, t)], p.astype(BF16), preferred_element_type=F32)
            pv = part if pv is None else pv + part
        mx_s[g_next][...] = top
        if first:
            l_s[g] = l_new
            acc_s[g] = pv
        else:
            l_s[g] = l_s[g] * alpha + l_new
            acc_s[g] = acc_s[g] * alpha + pv

    top = None
    for t in range(n_c):
        top = score_chunk(0, i, t, True, top)
    mx_s[0][...] = top
    for g in range(n_h):
        last = g == n_h - 1
        stage(g, i, True, 0 if last else g + 1, 0 if last else i, not last)

    def body(j, carry):
        for g in range(n_h):
            last = g == n_h - 1
            stage(g, j, False, 0 if last else g + 1, jnp.minimum(j + 1, i - 1) if last else j, False)
        return carry

    lax.fori_loop(0, i, body, 0)

    def moves(t, act):
        for n, out in enumerate(outs):
            r, p = n % n_tp, n // n_tp
            hit = ((t // per) ^ me) == r
            if n_parts == 1:
                dst = out.at[pl.ds(pl.multiple_of((t % per) * bq, bq), bq), :]
            else:
                dst = out
                hit = hit & (t % per == p)

            @pl.when(hit)
            def _(dst=dst):
                act(pltpu.make_async_copy(o_s, dst, sem))

    @pl.when(i > 0)
    def _():
        moves(i - 1, lambda copy: copy.wait())

    for g in range(n_h):
        l = jnp.sum(l_s[g], axis=0, keepdims=True)
        o_s[:, heads(g)] = (acc_s[g] / l).T.astype(BF16)
    moves(i, lambda copy: copy.start())

    @pl.when(i == n_q - 1)
    def _():
        moves(i, lambda copy: copy.wait())


def attn_call(q, k, vt, n_tp, n_parts):
    seq, cols = q.shape
    bq, ch, n_h = 512, 256, cols // HD
    size = seq // n_tp // n_parts
    return pl.pallas_call(
        functools.partial(attn_kernel, n_tp, n_parts, n_h, bq, ch),
        grid=(seq // bq,),
        in_specs=[pl.BlockSpec((bq, cols), lambda i: (i, 0)), pl.BlockSpec((seq, cols), lambda i: (0, 0)), pl.BlockSpec((cols, seq), lambda i: (0, 0))],
        out_specs=[pl.BlockSpec(memory_space=pl.ANY)] * (n_tp * n_parts),
        out_shape=[jax.ShapeDtypeStruct((size, cols), BF16)] * (n_tp * n_parts),
        scratch_shapes=[pltpu.VMEM((n_h, 8, bq), F32), pltpu.VMEM((n_h, HD, bq), F32), pltpu.VMEM((n_h, 1, bq), F32), pltpu.VMEM((bq, cols), BF16), pltpu.SemaphoreType.DMA]
        + [pltpu.VMEM((bq, bq), F32)] * n_h + [pltpu.VMEM((8, bq), F32)] * n_h,
        compiler_params=params("arbitrary"),
        cost_estimate=cost(4 * seq * seq * cols, 8 * seq * cols, seq * seq * cols // HD // 2),
        name="attn",
    )(q, k, vt)


def out_kernel(n_items, *refs):
    pieces, (w0, w1, w2, w3, x_ref) = refs[:4 * n_items], refs[4 * n_items:4 * n_items + 5]
    out_ref, o_buf, sems = refs[-3:]
    item, n = pl.program_id(0), pl.program_id(1)

    def loads(t):
        return [pltpu.make_async_copy(pieces[4 * t + r], o_buf.at[t % 2, r], sems.at[t % 2, r]) for r in range(4)]

    for t in range(n_items):
        @pl.when((item == max(t - 1, 0)) & (n == (1 if t else 0)))
        def _(t=t):
            for load in loads(t):
                load.start()

        @pl.when((item == t) & (n == 0))
        def _(t=t):
            for load in loads(t):
                load.wait()

    slot = item % 2
    acc = jnp.dot(o_buf[slot, 0], w0[...], preferred_element_type=F32)
    for r, w in ((1, w1), (2, w2), (3, w3)):
        acc += jnp.dot(o_buf[slot, r], w[...], preferred_element_type=F32)
    y = acc.astype(BF16).astype(F32)
    out_ref[0] = (x_ref[0].astype(F32) + y).astype(BF16)


def out_call(items, ws, x, prev, b, part):
    width = x.shape[2]
    n_items = len(items)
    rows, cols = items[0][0].shape
    bn = 512
    hbm = pl.BlockSpec(memory_space=pl.ANY)
    wspec = pl.BlockSpec((cols, bn), lambda t, n: (0, n))
    xspec = pl.BlockSpec((1, rows, bn), lambda t, n: (b + t, part, n))
    in_specs = [hbm] * (4 * n_items) + [wspec] * 4 + [xspec]
    args = [*sum(items, []), *ws, x]
    aliases = {}
    if prev is not None:
        aliases = {len(args): 0}
        in_specs.append(hbm)
        args.append(prev)
    return pl.pallas_call(
        functools.partial(out_kernel, n_items),
        grid=(n_items, width // bn),
        in_specs=in_specs,
        out_specs=xspec,
        out_shape=jax.ShapeDtypeStruct(x.shape, BF16),
        scratch_shapes=[pltpu.VMEM((2, 4, rows, cols), BF16), pltpu.SemaphoreType.DMA((2, 4))],
        input_output_aliases=aliases,
        compiler_params=params("arbitrary", "arbitrary"),
        cost_estimate=cost(2 * n_items * rows * width * width, n_items * (2 * width * width + 6 * rows * width)),
        name="outproj",
    )(*args)


def solution(mesh):
    n_tp = mesh.shape['tp']
    pairs = {r: [(d, d ^ r) for d in range(n_tp)] for r in range(1, n_tp)}

    def block(x_local, attn_gain, wq, wk, wv, qg, kg, wo_rows):
        n_batch, rows, width = x_local.shape
        seq = rows * n_tp
        cols = wq.shape[1]
        me = lax.axis_index('tp')
        ct, st = rope_tables(seq)

        qg, kg = qg.reshape(1, cols), kg.reshape(1, cols)
        me_arr = me.astype(jnp.int32).reshape(1)
        w_qkv = [wq, wk, wv]

        def after(val, *deps):
            return lax.optimization_barrier((val, *deps))[0]

        def send(val, hop):
            return lax.ppermute(val, 'tp', pairs[hop])

        gain = attn_gain.reshape(1, width)
        own = []
        for b in range(n_batch):
            own.append(norm_call(x_local, after(gain, own[-1][0]) if own else gain, b))
        far = [[None, None] for _ in own]

        def push(b, p, *deps):
            far[b][p] = send(after(own[b][p], *deps) if deps else own[b][p], 2)

        w_cut = [n * cols // 8 for n in (0, 4, 6, 8)]
        w2 = []

        def push_w(n, *deps):
            piece = (after(wo_rows, *deps) if deps else wo_rows)[w_cut[n]:w_cut[n + 1]]
            w2.append(send(piece, 2))
            return piece

        push(0, 0)
        push(0, 1)
        push(1, 0)
        near = [[send(h, 1) for h in parts] for parts in own]
        bufs, late, ex, stats = [], [], [], []
        vc = kc = out = ws = None

        def early(b, vc, *deps):
            n0 = after(near[b][0], *deps) if deps else near[b][0]
            buf, vc = qkv_call(me_arr, [*own[b], n0, near[b][1]], w_qkv, 0, None, vc, b, n_batch, seq)
            bufs.append(buf)
            return vc

        def project(b, vc, *deps):
            h30 = send(far[b][0], 1)
            f1 = after(far[b][1], *deps)
            h31 = send(f1, 1)
            buf, vc = qkv_call(me_arr, [far[b][0], f1, h30, h31], w_qkv, 2, bufs[b], vc, b, n_batch, seq)
            late.append(buf)
            stats.append(send(buf[3], 2))
            return vc

        def attend(b, kc, dep, n_parts=1):
            q, k, vt, ss = late[b]
            pair_ss = after(stats[b], dep) + ss
            tot = pair_ss + send(pair_ss, 1)
            qr, kr, kc = rope_call(q, k, tot, qg, kg, ct, st, kc, b, n_batch, width)
            o = attn_call(qr, kr, vt, n_tp, n_parts)
            return [o[p * n_tp:(p + 1) * n_tp] for p in range(n_parts)], kc

        def exchange(parts, dep=None):
            res = []
            for piece in parts:
                moved = [after(t, dep) if dep is not None else t for t in piece[1:]]
                res.append([piece[0]] + [send(t, r + 1) for r, t in enumerate(moved)])
            return res

        vc = early(0, None)
        vc = early(1, vc, vc, ct, st)
        vc = early(2, vc, vc)
        vc = project(0, vc, vc)
        done = late[0][3]
        push(1, 1, done)
        push(2, 0, done)
        vc = early(3, vc, done)
        push_w(0, done)
        o0, kc = attend(0, kc, vc)
        vc = project(1, vc, o0[0][0])
        done = late[1][3]
        push(2, 1, done)
        push(3, 0, done)
        mark = push_w(1, done)
        ex.append(exchange(o0, done))
        o1, kc = attend(1, kc, mark)
        vc = project(2, vc, o1[0][0])
        done = late[2][3]
        push(3, 1, done)
        mark = push_w(2, done)
        ex.append(exchange(o1, done))
        o2, kc = attend(2, kc, mark)
        vc = project(3, vc, o2[0][0])
        done = late[3][3]
        ex.append(exchange(o2, done))
        o3, kc = attend(3, kc, done, 2)
        ex.append(exchange(o3))
        w2 = jnp.concatenate([after(w2[0], o3[0][0]), *w2[1:]], axis=0)
        ws = [wo_rows, send(after(wo_rows, done), 1), w2, send(w2, 1)]
        first = [list(parts[0]) for parts in ex[:-1]]
        first[0][0] = after(first[0][0], ex[3][0][0])
        out = out_call(first, ws, x_local, None, 0, 0)
        for p, pos in enumerate(ex[-1]):
            out = out_call([pos], ws, x_local, out, n_batch - 1, p)
        shape = (n_batch, seq, cols // HD, HD)
        return (out, kc.reshape(shape), vc.reshape(shape))

    seq_spec = P('dp', 'tp', None)
    head_spec = P('dp', None, 'tp', None)
    col_spec = P(None, 'tp')
    return jax.shard_map(block, mesh=mesh, in_specs=(seq_spec, P(None), col_spec, col_spec, col_spec, P('tp'), P('tp'), P('tp', None)), out_specs=(seq_spec, head_spec, head_spec), check_vma=False)
```

```python
import functools
import math

import jax
import jax.numpy as jnp
from jax import lax
from jax.experimental import pallas as pl
from jax.experimental.pallas import tpu as pltpu
from jax.sharding import PartitionSpec as P


HD = 128
LOG2E = math.log2(math.e)
F32 = jnp.float32
BF16 = jnp.bfloat16
QKV_ROWS = 256
VMEM_LIMIT = 60 * 1024 * 1024


def params(*sem):
    return pltpu.CompilerParams(dimension_semantics=sem, vmem_limit_bytes=VMEM_LIMIT)


def cost(flops, nbytes, trans=0):
    return pl.CostEstimate(flops=int(flops), bytes_accessed=int(nbytes), transcendentals=int(trans))


def rope_tables(seq_len):
    fine = 64
    lane = jnp.arange(HD)
    inv_freq = 10000.0 ** (-(lane % (HD // 2)).astype(F32) * (2.0 / HD))
    low = jnp.arange(fine, dtype=F32)[:, None] * inv_freq[None, :]
    high = (jnp.arange(seq_len // fine) * fine).astype(F32)[:, None] * inv_freq[None, :]
    cl, sl, ch, sh = lax.optimization_barrier((jnp.cos(low)[None], jnp.sin(low)[None], jnp.cos(high)[:, None], jnp.sin(high)[:, None]))
    c = (ch * cl - sh * sl).reshape(seq_len, HD)
    s = (sh * cl + ch * sl).reshape(seq_len, HD)
    return c, jnp.where(lane < HD // 2, -s, s)


def sq_sum(a):
    part = None
    for g in range(a.shape[1] // HD):
        t = a[:, g * HD:(g + 1) * HD]
        part = t * t if part is None else part + t * t
    return jnp.sum(part.T, axis=0, keepdims=True)


def spread_heads(scr, blocks):
    n = len(blocks)
    rows = blocks[0].shape[0]
    for g, t in enumerate(blocks):
        scr[pl.ds(g, rows, stride=n), :] = t
    return scr[...].astype(BF16)


def norm_kernel(x_ref, g_ref, a_ref, b_ref):
    rows, width = a_ref.shape
    lower = pl.program_id(0) < pl.num_programs(0) // 2
    for first, dst in ((True, a_ref), (False, b_ref)):
        @pl.when(lower == first)
        def _(dst=dst):
            @pl.loop(0, rows // 64)
            def _(t):
                part = pl.ds(pl.multiple_of(t * 64, 64), 64)
                x = x_ref[0, part, :].astype(F32)
                mean = jnp.sum(x * x, axis=1, keepdims=True) * (1.0 / width)
                dst[part, :] = (x * lax.rsqrt(mean + 1e-5) * g_ref[...]).astype(BF16)


def norm_call(x, gain, b):
    rows, width = x.shape[1:]
    br = 256
    n = rows // br
    half = jax.ShapeDtypeStruct((rows // 2, width), BF16)
    return pl.pallas_call(
        norm_kernel,
        grid=(n,),
        in_specs=[pl.BlockSpec((1, br, width), lambda s: (b, s, 0)), pl.BlockSpec((1, width), lambda s: (0, 0))],
        out_specs=[pl.BlockSpec((br, width), lambda s: (jnp.minimum(s, n // 2 - 1), 0)), pl.BlockSpec((br, width), lambda s: (jnp.maximum(s - n // 2, 0), 0))],
        out_shape=[half, half],
        compiler_params=params("arbitrary"),
        cost_estimate=cost(8 * rows * width, 4 * rows * width),
        name="norm",
    )(x, gain)


def norm_half_kernel(x_ref, g_ref, h_ref):
    @pl.loop(0, h_ref.shape[0] // 64)
    def _(t):
        part = pl.ds(pl.multiple_of(t * 64, 64), 64)
        x = x_ref[0, part, :].astype(F32)
        mean = jnp.sum(x * x, axis=1, keepdims=True) * (1.0 / x.shape[1])
        h_ref[part, :] = (x * lax.rsqrt(mean + 1e-5) * g_ref[...]).astype(BF16)


def norm_half_call(x, gain, b, p):
    rows, width = x.shape[1:]
    br = 256
    n = rows // 2 // br
    return pl.pallas_call(
        norm_half_kernel,
        grid=(n,),
        in_specs=[pl.BlockSpec((1, br, width), lambda s: (b, p * n + s, 0)), pl.BlockSpec((1, width), lambda s: (0, 0))],
        out_specs=pl.BlockSpec((br, width), lambda s: (s, 0)),
        out_shape=jax.ShapeDtypeStruct((rows // 2, width), BF16),
        compiler_params=params("arbitrary"),
        cost_estimate=cost(4 * rows * width, 2 * rows * width),
        name="norm",
    )(x, gain)


def qkv_kernel(n_sub, me_ref, h0_ref, h1_ref, h2_ref, h3_ref, wq_ref, wk_ref, wv_ref, *refs):
    q_ref, k_ref, vt_ref, vc_ref, ss_ref, scr, h_ref = refs[-7:]
    step = pl.program_id(0)
    for n, src in enumerate((h0_ref, h1_ref, h2_ref, h3_ref)):
        @pl.when(step // n_sub == n)
        def _(src=src):
            @pl.loop(0, src.shape[0] // 64)
            def _(t):
                part = pl.ds(pl.multiple_of(t * 64, 64), 64)
                h_ref[part, :] = src[part, :]
    h = h_ref[...]
    cols = wq_ref.shape[1]
    q = jnp.dot(h, wq_ref[...], preferred_element_type=F32).astype(BF16)
    q_ref[...] = q
    k = jnp.dot(h, wk_ref[...], preferred_element_type=F32).astype(BF16)
    k_ref[...] = k
    ss_ref[0:1, :] = sq_sum(q.astype(F32))
    v = jnp.dot(h, wv_ref[...], preferred_element_type=F32)
    ss_ref[1:2, :] = sq_sum(k.astype(F32))
    vt_ref[...] = v.T.astype(BF16)
    vc_ref[...] = spread_heads(scr, [v[:, g * HD:(g + 1) * HD] for g in range(cols // HD)])


def qkv_call(me, hs, ws, r0, bufs, vc_prev, b, n_batch, seq):
    part, width = hs[0].shape
    cols = ws[0].shape[1]
    heads = cols // HD
    bq = QKV_ROWS
    n_sub = part // bq
    base = b * (seq // bq)

    def pos(s, m):
        return (m[0] ^ (r0 + s // (2 * n_sub))) * (2 * n_sub) + s % (2 * n_sub)

    def hspec(n):
        return pl.BlockSpec((bq, width), lambda s, m: (jnp.clip(s - n * n_sub, 0, n_sub - 1), 0))

    wspec = pl.BlockSpec((width, cols), lambda s, m: (0, 0))
    rspec = pl.BlockSpec((bq, cols), lambda s, m: (pos(s, m), 0))
    in_specs = [hspec(n) for n in range(4)] + [wspec, wspec, wspec]
    args = [me, *hs, *ws]
    aliases = {}
    for n, buf in enumerate([*(bufs or [None] * 4)[:3], vc_prev, (bufs or [None] * 4)[3]]):
        if buf is not None:
            aliases[len(args)] = n
            args.append(buf)
            in_specs.append(pl.BlockSpec(memory_space=pl.ANY))
    q, k, vt, vc, ss = pl.pallas_call(
        functools.partial(qkv_kernel, n_sub),
        grid_spec=pltpu.PrefetchScalarGridSpec(
            num_scalar_prefetch=1,
            grid=(4 * n_sub,),
            in_specs=in_specs,
            out_specs=[
                rspec, rspec,
                pl.BlockSpec((cols, bq), lambda s, m: (0, pos(s, m))),
                pl.BlockSpec((bq * heads, HD), lambda s, m: (base + pos(s, m), 0)),
                pl.BlockSpec((2, bq), lambda s, m: (0, pos(s, m))),
            ],
            scratch_shapes=[pltpu.VMEM((bq * heads, HD), F32), pltpu.VMEM((bq, width), BF16)],
        ),
        out_shape=[
            jax.ShapeDtypeStruct((seq, cols), BF16), jax.ShapeDtypeStruct((seq, cols), BF16), jax.ShapeDtypeStruct((cols, seq), BF16),
            jax.ShapeDtypeStruct((n_batch * seq * heads, HD), BF16), jax.ShapeDtypeStruct((2, seq), F32),
        ],
        input_output_aliases=aliases,
        compiler_params=params("arbitrary"),
        cost_estimate=cost(24 * part * width * cols, 8 * part * width + 6 * width * cols + 32 * part * cols),
        name="qkv",
    )(*args)
    return [q, k, vt, ss], vc


def rope_kernel(width, q_ref, k_ref, ss_ref, qg_ref, kg_ref, c_ref, s_ref, *refs):
    qr_ref, kr_ref, kc_ref, scr = refs[-4:]
    ct, st = c_ref[...], s_ref[...]
    rows = q_ref.shape[0]
    inv = lax.rsqrt(ss_ref[...] * (1.0 / width) + 1e-5)
    inv_t = jnp.concatenate([inv, jnp.zeros((6, rows), F32)], axis=0).T

    def turn(x_ref, col, g_ref):
        scale = inv_t[:, col:col + 1]
        outs = []
        for g in range(x_ref.shape[1] // HD):
            sl = slice(g * HD, (g + 1) * HD)
            n = x_ref[:, sl].astype(F32) * scale * g_ref[:, sl]
            outs.append(n * ct + pltpu.roll(n, HD // 2, 1) * st)
        return outs

    for g, t in enumerate(turn(q_ref, 0, qg_ref)):
        qr_ref[:, g * HD:(g + 1) * HD] = t.astype(BF16)
    ks = turn(k_ref, 1, kg_ref)
    for g, t in enumerate(ks):
        kr_ref[:, g * HD:(g + 1) * HD] = t.astype(BF16)
    kc_ref[...] = spread_heads(scr, ks)


def rope_call(q, k, ss, qg, kg, ct, st, kc_prev, b, n_batch, width):
    seq, cols = q.shape
    heads = cols // HD
    bq = 512
    nq = seq // bq
    rspec = pl.BlockSpec((bq, cols), lambda i: (i, 0))
    tspec = pl.BlockSpec((bq, HD), lambda i: (i, 0))
    gspec = pl.BlockSpec((1, cols), lambda i: (0, 0))
    in_specs = [rspec, rspec, pl.BlockSpec((2, bq), lambda i: (0, i)), gspec, gspec, tspec, tspec]
    args = [q, k, ss, qg, kg, ct, st]
    aliases = {}
    if kc_prev is not None:
        in_specs.append(pl.BlockSpec(memory_space=pl.ANY))
        args.append(kc_prev)
        aliases = {7: 2}
    base = b * nq
    return pl.pallas_call(
        functools.partial(rope_kernel, width),
        grid=(nq,),
        in_specs=in_specs,
        out_specs=[rspec, rspec, pl.BlockSpec((bq * heads, HD), lambda i: (base + i, 0))],
        out_shape=[jax.ShapeDtypeStruct((seq, cols), BF16)] * 2 + [jax.ShapeDtypeStruct((n_batch * seq * heads, HD), BF16)],
        scratch_shapes=[pltpu.VMEM((bq * heads, HD), F32)],
        input_output_aliases=aliases,
        compiler_params=params("arbitrary"),
        cost_estimate=cost(7e9, 10 * seq * cols),
        name="rope",
    )(*args)


def attn_kernel(n_tp, n_parts, n_h, bq, ch, q_ref, k_ref, vt_ref, *refs):
    outs = refs[:n_tp * n_parts]
    l_s, acc_s, m_s, o_s, sem, *stage_refs = refs[n_tp * n_parts:]
    me = lax.axis_index('tp')
    n_q = pl.num_programs(0)
    per = n_q // n_tp
    s_s, mx_s = stage_refs[:n_h], stage_refs[n_h:]
    i = pl.program_id(0)
    c = HD ** -0.5 * LOG2E
    n_c = bq // ch

    def heads(g):
        return slice(g * HD, (g + 1) * HD)

    def span(j, t):
        return pl.ds(pl.multiple_of(j * bq + t * ch, ch), ch)

    def score_chunk(g, j, t, diag, top):
        s = lax.dot_general(k_ref[span(j, t), heads(g)], q_ref[:, heads(g)], (((1,), (1,)), ((), ())), preferred_element_type=F32)
        if diag:
            k_pos = lax.broadcasted_iota(jnp.int32, (ch, bq), 0) + t * ch
            s = jnp.where(lax.broadcasted_iota(jnp.int32, (ch, bq), 1) >= k_pos, s, -1e30)
        s_s[g][t * ch:(t + 1) * ch, :] = s
        part = jnp.max(s.reshape(ch // 8, 8, bq), axis=0)
        return part if top is None else jnp.maximum(top, part)

    def stage(g, j, first, g_next, j_next, diag_next):
        m_new = jnp.max(mx_s[g][...], axis=0, keepdims=True) * c
        if not first:
            m_old = m_s[g]
            m_new = jnp.maximum(m_old, m_new)
            alpha = jnp.exp2(m_old - m_new)
        m_s[g] = m_new
        top = l_new = pv = None
        for t in range(n_c):
            top = score_chunk(g_next, j_next, t, diag_next, top)
            p = jnp.exp2(s_s[g][t * ch:(t + 1) * ch, :] * c - m_new)
            part = jnp.sum(p.reshape(ch // 8, 8, bq), axis=0)
            l_new = part if l_new is None else l_new + part
            part = jnp.dot(vt_ref[heads(g), span(j, t)], p.astype(BF16), preferred_element_type=F32)
            pv = part if pv is None else pv + part
        mx_s[g_next][...] = top
        if first:
            l_s[g] = l_new
            acc_s[g] = pv
        else:
            l_s[g] = l_s[g] * alpha + l_new
            acc_s[g] = acc_s[g] * alpha + pv

    top = None
    for t in range(n_c):
        top = score_chunk(0, i, t, True, top)
    mx_s[0][...] = top
    for g in range(n_h):
        last = g == n_h - 1
        stage(g, i, True, 0 if last else g + 1, 0 if last else i, not last)

    def body(j, carry):
        for g in range(n_h):
            last = g == n_h - 1
            stage(g, j, False, 0 if last else g + 1, jnp.minimum(j + 1, i - 1) if last else j, False)
        return carry

    lax.fori_loop(0, i, body, 0)

    def moves(t, act):
        for n, out in enumerate(outs):
            r, p = n % n_tp, n // n_tp
            hit = ((t // per) ^ me) == r
            if n_parts == 1:
                dst = out.at[pl.ds(pl.multiple_of((t % per) * bq, bq), bq), :]
            else:
                dst = out
                hit = hit & (t % per == p)

            @pl.when(hit)
            def _(dst=dst):
                act(pltpu.make_async_copy(o_s, dst, sem))

    @pl.when(i > 0)
    def _():
        moves(i - 1, lambda copy: copy.wait())

    for g in range(n_h):
        l = jnp.sum(l_s[g], axis=0, keepdims=True)
        o_s[:, heads(g)] = (acc_s[g] / l).T.astype(BF16)
    moves(i, lambda copy: copy.start())

    @pl.when(i == n_q - 1)
    def _():
        moves(i, lambda copy: copy.wait())


def attn_call(q, k, vt, n_tp, n_parts):
    seq, cols = q.shape
    bq, ch, n_h = 512, 256, cols // HD
    size = seq // n_tp // n_parts
    return pl.pallas_call(
        functools.partial(attn_kernel, n_tp, n_parts, n_h, bq, ch),
        grid=(seq // bq,),
        in_specs=[pl.BlockSpec((bq, cols), lambda i: (i, 0)), pl.BlockSpec((seq, cols), lambda i: (0, 0)), pl.BlockSpec((cols, seq), lambda i: (0, 0))],
        out_specs=[pl.BlockSpec(memory_space=pl.ANY)] * (n_tp * n_parts),
        out_shape=[jax.ShapeDtypeStruct((size, cols), BF16)] * (n_tp * n_parts),
        scratch_shapes=[pltpu.VMEM((n_h, 8, bq), F32), pltpu.VMEM((n_h, HD, bq), F32), pltpu.VMEM((n_h, 1, bq), F32), pltpu.VMEM((bq, cols), BF16), pltpu.SemaphoreType.DMA]
        + [pltpu.VMEM((bq, bq), F32)] * n_h + [pltpu.VMEM((8, bq), F32)] * n_h,
        compiler_params=params("arbitrary"),
        cost_estimate=cost(4 * seq * seq * cols, 8 * seq * cols, seq * seq * cols // HD // 2),
        name="attn",
    )(q, k, vt)


def out_kernel(n_items, *refs):
    pieces, (w0, w1, w2, w3, x_ref) = refs[:4 * n_items], refs[4 * n_items:4 * n_items + 5]
    out_ref, o_buf, sems = refs[-3:]
    item, n = pl.program_id(0), pl.program_id(1)

    def loads(t):
        return [pltpu.make_async_copy(pieces[4 * t + r], o_buf.at[t % 2, r], sems.at[t % 2, r]) for r in range(4)]

    for t in range(n_items):
        @pl.when((item == max(t - 1, 0)) & (n == (1 if t else 0)))
        def _(t=t):
            for load in loads(t):
                load.start()

        @pl.when((item == t) & (n == 0))
        def _(t=t):
            for load in loads(t):
                load.wait()

    slot = item % 2
    acc = jnp.dot(o_buf[slot, 0], w0[...], preferred_element_type=F32)
    for r, w in ((1, w1), (2, w2), (3, w3)):
        acc += jnp.dot(o_buf[slot, r], w[...], preferred_element_type=F32)
    y = acc.astype(BF16).astype(F32)
    out_ref[0] = (x_ref[0].astype(F32) + y).astype(BF16)


def out_call(items, ws, x, prev, b, part):
    width = x.shape[2]
    n_items = len(items)
    rows, cols = items[0][0].shape
    bn = 512
    hbm = pl.BlockSpec(memory_space=pl.ANY)
    wspec = pl.BlockSpec((cols, bn), lambda t, n: (0, n))
    xspec = pl.BlockSpec((1, rows, bn), lambda t, n: (b + t, part, n))
    in_specs = [hbm] * (4 * n_items) + [wspec] * 4 + [xspec]
    args = [*sum(items, []), *ws, x]
    aliases = {}
    if prev is not None:
        aliases = {len(args): 0}
        in_specs.append(hbm)
        args.append(prev)
    return pl.pallas_call(
        functools.partial(out_kernel, n_items),
        grid=(n_items, width // bn),
        in_specs=in_specs,
        out_specs=xspec,
        out_shape=jax.ShapeDtypeStruct(x.shape, BF16),
        scratch_shapes=[pltpu.VMEM((2, 4, rows, cols), BF16), pltpu.SemaphoreType.DMA((2, 4))],
        input_output_aliases=aliases,
        compiler_params=params("arbitrary", "arbitrary"),
        cost_estimate=cost(2 * n_items * rows * width * width, n_items * (2 * width * width + 6 * rows * width)),
        name="outproj",
    )(*args)


def near_kernel(o0_ref, o1_ref, w0_ref, w1_ref, acc_ref):
    acc = jnp.dot(o0_ref[...], w0_ref[...], preferred_element_type=F32)
    acc_ref[...] = acc + jnp.dot(o1_ref[...], w1_ref[...], preferred_element_type=F32)


def final_kernel(o2_ref, o3_ref, w2_ref, w3_ref, acc_ref, x_ref, *refs):
    acc = acc_ref[...] + jnp.dot(o2_ref[...], w2_ref[...], preferred_element_type=F32)
    acc += jnp.dot(o3_ref[...], w3_ref[...], preferred_element_type=F32)
    y = acc.astype(BF16).astype(F32)
    refs[-1][0] = (x_ref[0].astype(F32) + y).astype(BF16)


def half_out_call(pieces, ws, x=None, prev=None, acc=None, b=0, part=0):
    rows, cols = pieces[0].shape
    width = ws[0].shape[1]
    bn = 512
    ospec = pl.BlockSpec((rows, cols), lambda n: (0, 0))
    wspec = pl.BlockSpec((cols, bn), lambda n: (0, n))
    aspec = pl.BlockSpec((rows, bn), lambda n: (0, n))
    in_specs, args, aliases = [ospec] * 2 + [wspec] * 2, [*pieces, *ws], {}
    kernel, out_spec, out_shape = near_kernel, aspec, jax.ShapeDtypeStruct((rows, width), F32)
    if acc is not None:
        out_spec = pl.BlockSpec((1, rows, bn), lambda n: (b, part, n))
        in_specs += [aspec, out_spec, pl.BlockSpec(memory_space=pl.ANY)]
        args += [acc, x, prev]
        aliases = {6: 0}
        kernel, out_shape = final_kernel, jax.ShapeDtypeStruct(x.shape, BF16)
    return pl.pallas_call(
        kernel,
        grid=(width // bn,),
        in_specs=in_specs,
        out_specs=out_spec,
        out_shape=out_shape,
        input_output_aliases=aliases,
        compiler_params=params("arbitrary"),
        cost_estimate=cost(4 * rows * cols * width, 4 * cols * width + 8 * rows * width),
        name="outhalf",
    )(*args)


def solution(mesh):
    n_tp = mesh.shape['tp']
    pairs = {r: [(d, d ^ r) for d in range(n_tp)] for r in range(1, n_tp)}

    def block(x_local, attn_gain, wq, wk, wv, qg, kg, wo_rows):
        n_batch, rows, width = x_local.shape
        seq = rows * n_tp
        cols = wq.shape[1]
        me = lax.axis_index('tp')
        ct, st = rope_tables(seq)

        qg, kg = qg.reshape(1, cols), kg.reshape(1, cols)
        me_arr = me.astype(jnp.int32).reshape(1)
        w_qkv = [wq, wk, wv]

        def after(val, *deps):
            return lax.optimization_barrier((val, *deps))[0]

        def send(val, hop):
            return lax.ppermute(val, 'tp', pairs[hop])

        gain = attn_gain.reshape(1, width)
        own = [[norm_half_call(x_local, gain, 0, 0)]]
        own[0].append(norm_half_call(x_local, after(gain, own[0][0]), 0, 1))
        for b in range(1, n_batch):
            own.append(norm_call(x_local, after(gain, own[-1][1]), b))
        far = [[None, None] for _ in own]

        def push(b, p, *deps):
            far[b][p] = send(after(own[b][p], *deps) if deps else own[b][p], 2)

        w_cut = [n * cols // 8 for n in (0, 4, 6, 8)]
        w2 = []

        def push_w(n, *deps):
            piece = (after(wo_rows, *deps) if deps else wo_rows)[w_cut[n]:w_cut[n + 1]]
            w2.append(send(piece, 2))
            return piece

        push(0, 0)
        push(0, 1)
        push(1, 0)
        near = [[send(h, 1) for h in parts] for parts in own]
        bufs, late, ex, stats = [], [], [], []
        vc = kc = out = ws = None

        def early(b, vc, *deps):
            n0 = after(near[b][0], *deps) if deps else near[b][0]
            buf, vc = qkv_call(me_arr, [*own[b], n0, near[b][1]], w_qkv, 0, None, vc, b, n_batch, seq)
            bufs.append(buf)
            return vc

        def project(b, vc, *deps):
            h30 = send(far[b][0], 1)
            f1 = after(far[b][1], *deps)
            h31 = send(f1, 1)
            buf, vc = qkv_call(me_arr, [far[b][0], f1, h30, h31], w_qkv, 2, bufs[b], vc, b, n_batch, seq)
            late.append(buf)
            stats.append(send(buf[3], 2))
            return vc

        def attend(b, kc, dep, n_parts=1):
            q, k, vt, ss = late[b]
            pair_ss = after(stats[b], dep) + ss
            tot = pair_ss + send(pair_ss, 1)
            qr, kr, kc = rope_call(q, k, tot, qg, kg, ct, st, kc, b, n_batch, width)
            o = attn_call(qr, kr, vt, n_tp, n_parts)
            return [o[p * n_tp:(p + 1) * n_tp] for p in range(n_parts)], kc

        def exchange(parts, dep=None):
            res = []
            for piece in parts:
                moved = [after(t, dep) if dep is not None else t for t in piece[1:]]
                res.append([piece[0]] + [send(t, r + 1) for r, t in enumerate(moved)])
            return res

        def fill_w(n, buf, *deps):
            piece = after(w2[n], *deps)
            return lax.dynamic_update_slice(buf, piece, (w_cut[n], 0))

        vc = early(0, None)
        vc = early(1, vc, vc, ct, st)
        vc = early(2, vc, vc)
        vc = project(0, vc, vc)
        done = late[0][3]
        push(1, 1, done)
        push(2, 0, done)
        vc = early(3, vc, done)
        push_w(0, done)
        o0, kc = attend(0, kc, vc)
        vc = project(1, vc, o0[0][0])
        done = late[1][3]
        push(2, 1, done)
        push(3, 0, done)
        mark = push_w(1, done)
        ex.append(exchange(o0, done))
        o1, kc = attend(1, kc, mark)
        w_buf = fill_w(0, jnp.zeros((cols, width), BF16), o1[0][0])
        vc = project(2, vc, o1[0][0])
        done = late[2][3]
        push(3, 1, done)
        mark = push_w(2, done)
        ex.append(exchange(o1, done))
        o2, kc = attend(2, kc, mark)
        w_buf = fill_w(1, after(w_buf, o2[0][0]), o2[0][0])
        vc = project(3, vc, o2[0][0])
        done = late[3][3]
        ex.append(exchange(o2, done))
        o3, kc = attend(3, kc, done, 2)
        ex.append(exchange(o3))
        w2 = fill_w(2, w_buf, o3[0][0])
        ws = [wo_rows, send(after(wo_rows, done), 1), w2, send(w2, 1)]
        head, tail = ex[3]
        acc = half_out_call(tail[:2], ws[:2])
        first = [list(parts[0]) for parts in ex[:-1]]
        first[0][0] = after(first[0][0], acc)
        out = out_call(first, ws, x_local, None, 0, 0)
        out = out_call([head], ws, x_local, out, n_batch - 1, 0)
        out = half_out_call(tail[2:], ws[2:], x_local, out, acc, n_batch - 1, 1)
        shape = (n_batch, seq, cols // HD, HD)
        return (out, kc.reshape(shape), vc.reshape(shape))

    seq_spec = P('dp', 'tp', None)
    head_spec = P('dp', None, 'tp', None)
    col_spec = P(None, 'tp')
    return jax.shard_map(block, mesh=mesh, in_specs=(seq_spec, P(None), col_spec, col_spec, col_spec, P('tp'), P('tp'), P('tp', None)), out_specs=(seq_spec, head_spec, head_spec), check_vma=False)
```

```python
import functools
import math

import jax
import jax.numpy as jnp
from jax import lax
from jax.experimental import pallas as pl
from jax.experimental.pallas import tpu as pltpu
from jax.sharding import PartitionSpec as P


HD = 128
LOG2E = math.log2(math.e)
F32 = jnp.float32
BF16 = jnp.bfloat16
QKV_ROWS = 256
OUT_LIMIT = 48 * 1024 * 1024
VMEM_LIMIT = 60 * 1024 * 1024


def params(*sem, limit=VMEM_LIMIT):
    return pltpu.CompilerParams(dimension_semantics=sem, vmem_limit_bytes=limit)


def cost(flops, nbytes, trans=0):
    return pl.CostEstimate(flops=int(flops), bytes_accessed=int(nbytes), transcendentals=int(trans))


def rope_tables(seq_len):
    fine = 64
    lane = jnp.arange(HD)
    inv_freq = 10000.0 ** (-(lane % (HD // 2)).astype(F32) * (2.0 / HD))
    low = jnp.arange(fine, dtype=F32)[:, None] * inv_freq[None, :]
    high = (jnp.arange(seq_len // fine) * fine).astype(F32)[:, None] * inv_freq[None, :]
    cl, sl, ch, sh = lax.optimization_barrier((jnp.cos(low)[None], jnp.sin(low)[None], jnp.cos(high)[:, None], jnp.sin(high)[:, None]))
    c = (ch * cl - sh * sl).reshape(seq_len, HD)
    s = (sh * cl + ch * sl).reshape(seq_len, HD)
    return c, jnp.where(lane < HD // 2, -s, s)


def sq_sum(a):
    part = None
    for g in range(a.shape[1] // HD):
        t = a[:, g * HD:(g + 1) * HD]
        part = t * t if part is None else part + t * t
    return jnp.sum(part.T, axis=0, keepdims=True)


def spread_heads(scr, blocks):
    n = len(blocks)
    rows = blocks[0].shape[0]
    for g, t in enumerate(blocks):
        scr[pl.ds(g, rows, stride=n), :] = t
    return scr[...].astype(BF16)


def norm_kernel(x_ref, g_ref, a_ref, b_ref):
    rows, width = a_ref.shape
    lower = pl.program_id(0) < pl.num_programs(0) // 2
    for first, dst in ((True, a_ref), (False, b_ref)):
        @pl.when(lower == first)
        def _(dst=dst):
            @pl.loop(0, rows // 64)
            def _(t):
                part = pl.ds(pl.multiple_of(t * 64, 64), 64)
                x = x_ref[0, part, :].astype(F32)
                mean = jnp.sum(x * x, axis=1, keepdims=True) * (1.0 / width)
                dst[part, :] = (x * lax.rsqrt(mean + 1e-5) * g_ref[...]).astype(BF16)


def norm_call(x, gain, b):
    rows, width = x.shape[1:]
    br = 256
    n = rows // br
    half = jax.ShapeDtypeStruct((rows // 2, width), BF16)
    return pl.pallas_call(
        norm_kernel,
        grid=(n,),
        in_specs=[pl.BlockSpec((1, br, width), lambda s: (b, s, 0)), pl.BlockSpec((1, width), lambda s: (0, 0))],
        out_specs=[pl.BlockSpec((br, width), lambda s: (jnp.minimum(s, n // 2 - 1), 0)), pl.BlockSpec((br, width), lambda s: (jnp.maximum(s - n // 2, 0), 0))],
        out_shape=[half, half],
        compiler_params=params("arbitrary"),
        cost_estimate=cost(8 * rows * width, 4 * rows * width),
        name="norm",
    )(x, gain)


def norm_half_kernel(x_ref, g_ref, h_ref):
    @pl.loop(0, h_ref.shape[0] // 64)
    def _(t):
        part = pl.ds(pl.multiple_of(t * 64, 64), 64)
        x = x_ref[0, part, :].astype(F32)
        mean = jnp.sum(x * x, axis=1, keepdims=True) * (1.0 / x.shape[1])
        h_ref[part, :] = (x * lax.rsqrt(mean + 1e-5) * g_ref[...]).astype(BF16)


def norm_half_call(x, gain, b, p):
    rows, width = x.shape[1:]
    br = 256
    n = rows // 2 // br
    return pl.pallas_call(
        norm_half_kernel,
        grid=(n,),
        in_specs=[pl.BlockSpec((1, br, width), lambda s: (b, p * n + s, 0)), pl.BlockSpec((1, width), lambda s: (0, 0))],
        out_specs=pl.BlockSpec((br, width), lambda s: (s, 0)),
        out_shape=jax.ShapeDtypeStruct((rows // 2, width), BF16),
        compiler_params=params("arbitrary"),
        cost_estimate=cost(4 * rows * width, 2 * rows * width),
        name="norm",
    )(x, gain)


def qkv_kernel(n_sub, me_ref, h0_ref, h1_ref, h2_ref, h3_ref, wq_ref, wk_ref, wv_ref, *refs):
    q_ref, k_ref, vt_ref, vc_ref, ss_ref, scr, h_ref = refs[-7:]
    step = pl.program_id(0)
    for n, src in enumerate((h0_ref, h1_ref, h2_ref, h3_ref)):
        @pl.when(step // n_sub == n)
        def _(src=src):
            @pl.loop(0, src.shape[0] // 64)
            def _(t):
                part = pl.ds(pl.multiple_of(t * 64, 64), 64)
                h_ref[part, :] = src[part, :]
    h = h_ref[...]
    cols = wq_ref.shape[1]
    q = jnp.dot(h, wq_ref[...], preferred_element_type=F32).astype(BF16)
    q_ref[...] = q
    k = jnp.dot(h, wk_ref[...], preferred_element_type=F32).astype(BF16)
    k_ref[...] = k
    ss_ref[0:1, :] = sq_sum(q.astype(F32))
    v = jnp.dot(h, wv_ref[...], preferred_element_type=F32)
    ss_ref[1:2, :] = sq_sum(k.astype(F32))
    vt_ref[...] = v.T.astype(BF16)
    vc_ref[...] = spread_heads(scr, [v[:, g * HD:(g + 1) * HD] for g in range(cols // HD)])


def qkv_call(me, hs, ws, r0, bufs, vc_prev, b, n_batch, seq):
    part, width = hs[0].shape
    cols = ws[0].shape[1]
    heads = cols // HD
    bq = QKV_ROWS
    n_sub = part // bq
    base = b * (seq // bq)

    def pos(s, m):
        return (m[0] ^ (r0 + s // (2 * n_sub))) * (2 * n_sub) + s % (2 * n_sub)

    def hspec(n):
        return pl.BlockSpec((bq, width), lambda s, m: (jnp.clip(s - n * n_sub, 0, n_sub - 1), 0))

    wspec = pl.BlockSpec((width, cols), lambda s, m: (0, 0))
    rspec = pl.BlockSpec((bq, cols), lambda s, m: (pos(s, m), 0))
    in_specs = [hspec(n) for n in range(4)] + [wspec, wspec, wspec]
    args = [me, *hs, *ws]
    aliases = {}
    for n, buf in enumerate([*(bufs or [None] * 4)[:3], vc_prev, (bufs or [None] * 4)[3]]):
        if buf is not None:
            aliases[len(args)] = n
            args.append(buf)
            in_specs.append(pl.BlockSpec(memory_space=pl.ANY))
    q, k, vt, vc, ss = pl.pallas_call(
        functools.partial(qkv_kernel, n_sub),
        grid_spec=pltpu.PrefetchScalarGridSpec(
            num_scalar_prefetch=1,
            grid=(4 * n_sub,),
            in_specs=in_specs,
            out_specs=[
                rspec, rspec,
                pl.BlockSpec((cols, bq), lambda s, m: (0, pos(s, m))),
                pl.BlockSpec((bq * heads, HD), lambda s, m: (base + pos(s, m), 0)),
                pl.BlockSpec((2, bq), lambda s, m: (0, pos(s, m))),
            ],
            scratch_shapes=[pltpu.VMEM((bq * heads, HD), F32), pltpu.VMEM((bq, width), BF16)],
        ),
        out_shape=[
            jax.ShapeDtypeStruct((seq, cols), BF16), jax.ShapeDtypeStruct((seq, cols), BF16), jax.ShapeDtypeStruct((cols, seq), BF16),
            jax.ShapeDtypeStruct((n_batch * seq * heads, HD), BF16), jax.ShapeDtypeStruct((2, seq), F32),
        ],
        input_output_aliases=aliases,
        compiler_params=params("arbitrary"),
        cost_estimate=cost(24 * part * width * cols, 8 * part * width + 6 * width * cols + 32 * part * cols),
        name="qkv",
    )(*args)
    return [q, k, vt, ss], vc


def rope_kernel(width, q_ref, k_ref, ss_ref, qg_ref, kg_ref, c_ref, s_ref, *refs):
    qr_ref, kr_ref, kc_ref, scr = refs[-4:]
    ct, st = c_ref[...], s_ref[...]
    rows = q_ref.shape[0]
    inv = lax.rsqrt(ss_ref[...] * (1.0 / width) + 1e-5)
    inv_t = jnp.concatenate([inv, jnp.zeros((6, rows), F32)], axis=0).T

    def turn(x_ref, col, g_ref):
        scale = inv_t[:, col:col + 1]
        outs = []
        for g in range(x_ref.shape[1] // HD):
            sl = slice(g * HD, (g + 1) * HD)
            n = x_ref[:, sl].astype(F32) * scale * g_ref[:, sl]
            outs.append(n * ct + pltpu.roll(n, HD // 2, 1) * st)
        return outs

    for g, t in enumerate(turn(q_ref, 0, qg_ref)):
        qr_ref[:, g * HD:(g + 1) * HD] = t.astype(BF16)
    ks = turn(k_ref, 1, kg_ref)
    for g, t in enumerate(ks):
        kr_ref[:, g * HD:(g + 1) * HD] = t.astype(BF16)
    kc_ref[...] = spread_heads(scr, ks)


def rope_call(q, k, ss, qg, kg, ct, st, kc_prev, b, n_batch, width):
    seq, cols = q.shape
    heads = cols // HD
    bq = 512
    nq = seq // bq
    rspec = pl.BlockSpec((bq, cols), lambda i: (i, 0))
    tspec = pl.BlockSpec((bq, HD), lambda i: (i, 0))
    gspec = pl.BlockSpec((1, cols), lambda i: (0, 0))
    in_specs = [rspec, rspec, pl.BlockSpec((2, bq), lambda i: (0, i)), gspec, gspec, tspec, tspec]
    args = [q, k, ss, qg, kg, ct, st]
    aliases = {}
    if kc_prev is not None:
        in_specs.append(pl.BlockSpec(memory_space=pl.ANY))
        args.append(kc_prev)
        aliases = {7: 2}
    base = b * nq
    return pl.pallas_call(
        functools.partial(rope_kernel, width),
        grid=(nq,),
        in_specs=in_specs,
        out_specs=[rspec, rspec, pl.BlockSpec((bq * heads, HD), lambda i: (base + i, 0))],
        out_shape=[jax.ShapeDtypeStruct((seq, cols), BF16)] * 2 + [jax.ShapeDtypeStruct((n_batch * seq * heads, HD), BF16)],
        scratch_shapes=[pltpu.VMEM((bq * heads, HD), F32)],
        input_output_aliases=aliases,
        compiler_params=params("arbitrary"),
        cost_estimate=cost(7e9, 10 * seq * cols),
        name="rope",
    )(*args)


def attn_kernel(n_tp, n_parts, n_h, bq, ch, q_ref, k_ref, vt_ref, *refs):
    outs = refs[:n_tp * n_parts]
    l_s, acc_s, m_s, o_s, sem, *stage_refs = refs[n_tp * n_parts:]
    me = lax.axis_index('tp')
    n_q = pl.num_programs(0)
    per = n_q // n_tp
    s_s, mx_s = stage_refs[:n_h], stage_refs[n_h:]
    i = pl.program_id(0)
    c = HD ** -0.5 * LOG2E
    n_c = bq // ch

    def heads(g):
        return slice(g * HD, (g + 1) * HD)

    def span(j, t):
        return pl.ds(pl.multiple_of(j * bq + t * ch, ch), ch)

    def score_chunk(g, j, t, diag, top):
        s = lax.dot_general(k_ref[span(j, t), heads(g)], q_ref[:, heads(g)], (((1,), (1,)), ((), ())), preferred_element_type=F32)
        if diag:
            k_pos = lax.broadcasted_iota(jnp.int32, (ch, bq), 0) + t * ch
            s = jnp.where(lax.broadcasted_iota(jnp.int32, (ch, bq), 1) >= k_pos, s, -1e30)
        s_s[g][t * ch:(t + 1) * ch, :] = s
        part = jnp.max(s.reshape(ch // 8, 8, bq), axis=0)
        return part if top is None else jnp.maximum(top, part)

    def stage(g, j, first, g_next, j_next, diag_next):
        m_new = jnp.max(mx_s[g][...], axis=0, keepdims=True) * c
        if not first:
            m_old = m_s[g]
            m_new = jnp.maximum(m_old, m_new)
            alpha = jnp.exp2(m_old - m_new)
        m_s[g] = m_new
        top = l_new = pv = None
        for t in range(n_c):
            top = score_chunk(g_next, j_next, t, diag_next, top)
            p = jnp.exp2(s_s[g][t * ch:(t + 1) * ch, :] * c - m_new)
            part = jnp.sum(p.reshape(ch // 8, 8, bq), axis=0)
            l_new = part if l_new is None else l_new + part
            part = jnp.dot(vt_ref[heads(g), span(j, t)], p.astype(BF16), preferred_element_type=F32)
            pv = part if pv is None else pv + part
        mx_s[g_next][...] = top
        if first:
            l_s[g] = l_new
            acc_s[g] = pv
        else:
            l_s[g] = l_s[g] * alpha + l_new
            acc_s[g] = acc_s[g] * alpha + pv

    top = None
    for t in range(n_c):
        top = score_chunk(0, i, t, True, top)
    mx_s[0][...] = top
    for g in range(n_h):
        last = g == n_h - 1
        stage(g, i, True, 0 if last else g + 1, 0 if last else i, not last)

    def body(j, carry):
        for g in range(n_h):
            last = g == n_h - 1
            stage(g, j, False, 0 if last else g + 1, jnp.minimum(j + 1, i - 1) if last else j, False)
        return carry

    lax.fori_loop(0, i, body, 0)

    def moves(t, act):
        for n, out in enumerate(outs):
            r, p = n % n_tp, n // n_tp
            hit = ((t // per) ^ me) == r
            if n_parts == 1:
                dst = out.at[pl.ds(pl.multiple_of((t % per) * bq, bq), bq), :]
            else:
                dst = out
                hit = hit & (t % per == p)

            @pl.when(hit)
            def _(dst=dst):
                act(pltpu.make_async_copy(o_s, dst, sem))

    @pl.when(i > 0)
    def _():
        moves(i - 1, lambda copy: copy.wait())

    for g in range(n_h):
        l = jnp.sum(l_s[g], axis=0, keepdims=True)
        o_s[:, heads(g)] = (acc_s[g] / l).T.astype(BF16)
    moves(i, lambda copy: copy.start())

    @pl.when(i == n_q - 1)
    def _():
        moves(i, lambda copy: copy.wait())


def attn_call(q, k, vt, n_tp, n_parts):
    seq, cols = q.shape
    bq, ch, n_h = 512, 256, cols // HD
    size = seq // n_tp // n_parts
    return pl.pallas_call(
        functools.partial(attn_kernel, n_tp, n_parts, n_h, bq, ch),
        grid=(seq // bq,),
        in_specs=[pl.BlockSpec((bq, cols), lambda i: (i, 0)), pl.BlockSpec((seq, cols), lambda i: (0, 0)), pl.BlockSpec((cols, seq), lambda i: (0, 0))],
        out_specs=[pl.BlockSpec(memory_space=pl.ANY)] * (n_tp * n_parts),
        out_shape=[jax.ShapeDtypeStruct((size, cols), BF16)] * (n_tp * n_parts),
        scratch_shapes=[pltpu.VMEM((n_h, 8, bq), F32), pltpu.VMEM((n_h, HD, bq), F32), pltpu.VMEM((n_h, 1, bq), F32), pltpu.VMEM((bq, cols), BF16), pltpu.SemaphoreType.DMA]
        + [pltpu.VMEM((bq, bq), F32)] * n_h + [pltpu.VMEM((8, bq), F32)] * n_h,
        compiler_params=params("arbitrary"),
        cost_estimate=cost(4 * seq * seq * cols, 8 * seq * cols, seq * seq * cols // HD // 2),
        name="attn",
    )(q, k, vt)


def out_kernel(n_items, *refs):
    pieces, (w0, w1, w2, w3, x_ref) = refs[:4 * n_items], refs[4 * n_items:4 * n_items + 5]
    out_ref, o_buf, sems = refs[-3:]
    item, n = pl.program_id(0), pl.program_id(1)

    def loads(t):
        return [pltpu.make_async_copy(pieces[4 * t + r], o_buf.at[t % 2, r], sems.at[t % 2, r]) for r in range(4)]

    for t in range(n_items):
        @pl.when((item == max(t - 1, 0)) & (n == (1 if t else 0)))
        def _(t=t):
            for load in loads(t):
                load.start()

        @pl.when((item == t) & (n == 0))
        def _(t=t):
            for load in loads(t):
                load.wait()

    slot = item % 2
    acc = jnp.dot(o_buf[slot, 0], w0[...], preferred_element_type=F32)
    for r, w in ((1, w1), (2, w2), (3, w3)):
        acc += jnp.dot(o_buf[slot, r], w[...], preferred_element_type=F32)
    y = acc.astype(BF16).astype(F32)
    out_ref[0] = (x_ref[0].astype(F32) + y).astype(BF16)


def out_call(items, ws, x, prev, b, part):
    width = x.shape[2]
    n_items = len(items)
    rows, cols = items[0][0].shape
    bn = 512
    hbm = pl.BlockSpec(memory_space=pl.ANY)
    wspec = pl.BlockSpec((cols, bn), lambda t, n: (0, n))
    xspec = pl.BlockSpec((1, rows, bn), lambda t, n: (b + t, part, n))
    in_specs = [hbm] * (4 * n_items) + [wspec] * 4 + [xspec]
    args = [*sum(items, []), *ws, x]
    aliases = {}
    if prev is not None:
        aliases = {len(args): 0}
        in_specs.append(hbm)
        args.append(prev)
    return pl.pallas_call(
        functools.partial(out_kernel, n_items),
        grid=(n_items, width // bn),
        in_specs=in_specs,
        out_specs=xspec,
        out_shape=jax.ShapeDtypeStruct(x.shape, BF16),
        scratch_shapes=[pltpu.VMEM((2, 4, rows, cols), BF16), pltpu.SemaphoreType.DMA((2, 4))],
        input_output_aliases=aliases,
        compiler_params=params("arbitrary", "arbitrary", limit=OUT_LIMIT),
        cost_estimate=cost(2 * n_items * rows * width * width, n_items * (2 * width * width + 6 * rows * width)),
        name="outproj",
    )(*args)


def near_kernel(o0_ref, o1_ref, w0_ref, w1_ref, acc_ref):
    acc = jnp.dot(o0_ref[...], w0_ref[...], preferred_element_type=F32)
    acc_ref[...] = acc + jnp.dot(o1_ref[...], w1_ref[...], preferred_element_type=F32)


def final_kernel(o2_ref, o3_ref, w2_ref, w3_ref, acc_ref, x_ref, *refs):
    acc = acc_ref[...] + jnp.dot(o2_ref[...], w2_ref[...], preferred_element_type=F32)
    acc += jnp.dot(o3_ref[...], w3_ref[...], preferred_element_type=F32)
    y = acc.astype(BF16).astype(F32)
    refs[-1][0] = (x_ref[0].astype(F32) + y).astype(BF16)


def half_out_call(pieces, ws, x=None, prev=None, acc=None, b=0, part=0):
    rows, cols = pieces[0].shape
    width = ws[0].shape[1]
    bn = 512
    ospec = pl.BlockSpec((rows, cols), lambda n: (0, 0))
    wspec = pl.BlockSpec((cols, bn), lambda n: (0, n))
    aspec = pl.BlockSpec((rows, bn), lambda n: (0, n))
    in_specs, args, aliases = [ospec] * 2 + [wspec] * 2, [*pieces, *ws], {}
    kernel, out_spec, out_shape = near_kernel, aspec, jax.ShapeDtypeStruct((rows, width), F32)
    if acc is not None:
        out_spec = pl.BlockSpec((1, rows, bn), lambda n: (b, part, n))
        in_specs += [aspec, out_spec, pl.BlockSpec(memory_space=pl.ANY)]
        args += [acc, x, prev]
        aliases = {6: 0}
        kernel, out_shape = final_kernel, jax.ShapeDtypeStruct(x.shape, BF16)
    return pl.pallas_call(
        kernel,
        grid=(width // bn,),
        in_specs=in_specs,
        out_specs=out_spec,
        out_shape=out_shape,
        input_output_aliases=aliases,
        compiler_params=params("arbitrary", limit=OUT_LIMIT),
        cost_estimate=cost(4 * rows * cols * width, 4 * cols * width + 8 * rows * width),
        name="outhalf",
    )(*args)


def solution(mesh):
    n_tp = mesh.shape['tp']
    pairs = {r: [(d, d ^ r) for d in range(n_tp)] for r in range(1, n_tp)}

    def block(x_local, attn_gain, wq, wk, wv, qg, kg, wo_rows):
        n_batch, rows, width = x_local.shape
        seq = rows * n_tp
        cols = wq.shape[1]
        me = lax.axis_index('tp')
        ct, st = rope_tables(seq)

        qg, kg = qg.reshape(1, cols), kg.reshape(1, cols)
        me_arr = me.astype(jnp.int32).reshape(1)
        w_qkv = [wq, wk, wv]

        def after(val, *deps):
            return lax.optimization_barrier((val, *deps))[0]

        def send(val, hop):
            return lax.ppermute(val, 'tp', pairs[hop])

        gain = attn_gain.reshape(1, width)
        own = [[norm_half_call(x_local, gain, 0, 0)]]
        own[0].append(norm_half_call(x_local, after(gain, own[0][0]), 0, 1))
        for b in range(1, n_batch):
            own.append(norm_call(x_local, after(gain, own[-1][1]), b))
        far = [[None, None] for _ in own]

        def push(b, p, *deps):
            far[b][p] = send(after(own[b][p], *deps) if deps else own[b][p], 2)

        w_cut = [n * cols // 8 for n in (0, 4, 6, 8)]
        w2 = []

        def push_w(n, *deps):
            piece = (after(wo_rows, *deps) if deps else wo_rows)[w_cut[n]:w_cut[n + 1]]
            w2.append(send(piece, 2))
            return piece

        push(0, 0)
        push(0, 1)
        push(1, 0)
        near = [[send(h, 1) for h in parts] for parts in own]
        bufs, late, ex, stats = [], [], [], []
        vc = kc = out = ws = None

        def early(b, vc, *deps):
            n0 = after(near[b][0], *deps) if deps else near[b][0]
            buf, vc = qkv_call(me_arr, [*own[b], n0, near[b][1]], w_qkv, 0, None, vc, b, n_batch, seq)
            bufs.append(buf)
            return vc

        def project(b, vc, *deps):
            h30 = send(far[b][0], 1)
            f1 = after(far[b][1], *deps)
            h31 = send(f1, 1)
            buf, vc = qkv_call(me_arr, [far[b][0], f1, h30, h31], w_qkv, 2, bufs[b], vc, b, n_batch, seq)
            late.append(buf)
            stats.append(send(buf[3], 2))
            return vc

        def attend(b, kc, dep, n_parts=1):
            q, k, vt, ss = late[b]
            pair_ss = after(stats[b], dep) + ss
            tot = pair_ss + send(pair_ss, 1)
            qr, kr, kc = rope_call(q, k, tot, qg, kg, ct, st, kc, b, n_batch, width)
            o = attn_call(qr, kr, vt, n_tp, n_parts)
            return [o[p * n_tp:(p + 1) * n_tp] for p in range(n_parts)], kc

        def exchange(parts, dep=None):
            res = []
            for piece in parts:
                moved = [after(t, dep) if dep is not None else t for t in piece[1:]]
                res.append([piece[0]] + [send(t, r + 1) for r, t in enumerate(moved)])
            return res

        def fill_w(n, buf, *deps):
            piece = after(w2[n], *deps)
            return lax.dynamic_update_slice(buf, piece, (w_cut[n], 0))

        vc = early(0, None)
        vc = early(1, vc, vc, ct, st)
        vc = early(2, vc, vc)
        vc = project(0, vc, vc)
        done = late[0][3]
        push(1, 1, done)
        push(2, 0, done)
        vc = early(3, vc, done)
        push_w(0, done)
        o0, kc = attend(0, kc, vc)
        vc = project(1, vc, o0[0][0])
        done = late[1][3]
        push(2, 1, done)
        push(3, 0, done)
        mark = push_w(1, done)
        ex.append(exchange(o0, done))
        o1, kc = attend(1, kc, mark)
        w_buf = fill_w(0, jnp.zeros((cols, width), BF16), o1[0][0])
        vc = project(2, vc, o1[0][0])
        done = late[2][3]
        push(3, 1, done)
        mark = push_w(2, done)
        ex.append(exchange(o1, done))
        o2, kc = attend(2, kc, mark)
        w_buf = fill_w(1, after(w_buf, o2[0][0]), o2[0][0])
        vc = project(3, vc, o2[0][0])
        done = late[3][3]
        ex.append(exchange(o2, done))
        o3, kc = attend(3, kc, done, 2)
        ex.append(exchange(o3))
        w2 = fill_w(2, w_buf, o3[0][0])
        ws = [wo_rows, send(after(wo_rows, done), 1), w2, send(w2, 1)]
        head, tail = ex[3]
        acc = half_out_call(tail[:2], ws[:2])
        first = [list(parts[0]) for parts in ex[:-1]]
        first[0][0] = after(first[0][0], acc)
        out = out_call(first, ws, x_local, None, 0, 0)
        out = out_call([head], ws, x_local, out, n_batch - 1, 0)
        out = half_out_call(tail[2:], ws[2:], x_local, out, acc, n_batch - 1, 1)
        shape = (n_batch, seq, cols // HD, HD)
        return (out, kc.reshape(shape), vc.reshape(shape))

    seq_spec = P('dp', 'tp', None)
    head_spec = P('dp', None, 'tp', None)
    col_spec = P(None, 'tp')
    return jax.shard_map(block, mesh=mesh, in_specs=(seq_spec, P(None), col_spec, col_spec, col_spec, P('tp'), P('tp'), P('tp', None)), out_specs=(seq_spec, head_spec, head_spec), check_vma=False)
```
